512 devices in a mesh: head: 4 (over y), tok: 32 (over z, core), hid: 4 (over x).
Axes of the slice: x: 4, y: 4, z: 16, core: 2. Of those that a mesh axis runs over, the one named last changes fastest.
Arguments:
- queries: bfloat16 [16384, 4096], P('tok', 'head'), may hold values from -12 to 12
- keys: bfloat16 [16384, 4096], P('tok', 'head'), may hold values from -12 to 12
- values: bfloat16 [16384, 4096], P('tok', 'head'), may hold values from -12 to 12
- token_rate: float32 [16384, 8], P('tok', 'head'), may hold values from 0.05 to 1
- head_rate: float32 [8], P('head'), may hold values from 0.2 to 1
- w_gate: bfloat16 [8, 512, 1024], P('head', None, 'hid'), may hold values from -0.25 to 0.25
- w_up: bfloat16 [8, 512, 1024], P('head', None, 'hid'), may hold values from -0.25 to 0.25
- w_down: bfloat16 [8, 1024, 512], P('head', 'hid'), may hold values from -0.25 to 0.25
Outputs:
- result: bfloat16 [16384, 4096], P('tok', ('head', 'hid'))
The draws below stay inside these ranges and needn't reach their ends.
All inputs are finite; a program needn't handle non-finite values.
Results may differ from the reference program's by a relative error of at most 0.035.
Values may be sent and summed in bfloat16 or wider, within the bound.
No kernel may reach another device: no remote copies, remote signals or barrier semaphores. Data moves between devices by JAX's collectives and lax.ppermute only.
A program may use at most 64 MiB of HBM per device.

```python
import math
import jax
import jax.numpy as jnp
from jax import lax

DH = 512
FH = 1024
NS_ITERS = 3
HEADS = 8
TOKENS = 16384
N_HID = 4


def offset_vector(base_key, salt):
    sign_key, size_key = jax.random.split(jax.random.fold_in(base_key, salt), 2)
    amplitude = 0.3
    signs = jnp.where(jax.random.bernoulli(sign_key, 0.5, (HEADS * DH,)), 1.0, -1.0)
    sizes = jax.random.uniform(size_key, (HEADS * DH,), minval=0.5, maxval=1.5)
    return (signs * sizes * amplitude).astype(jnp.float32)


def channel_draw(base_key, shift):
    first_key, second_key = jax.random.split(base_key, 2)
    channel = (jnp.arange(HEADS * DH) % DH).astype(jnp.float32)
    jitter = jnp.exp(jax.random.uniform(second_key, (HEADS * DH,), minval=math.log(0.7), maxval=math.log(1.4)))
    ramp = 10.0 ** (0.5 * channel / DH - 0.25)
    basic = jax.random.truncated_normal(first_key, -4.0, 4.0, (TOKENS, HEADS * DH))
    return jnp.clip(basic * ramp * jitter + shift[None, :], -12.0, 12.0).astype(jnp.bfloat16)


def draw_queries(key, part):
    return channel_draw(jax.random.fold_in(key, 37), offset_vector(key, 5))


def draw_keys(key, part):
    return channel_draw(jax.random.fold_in(key, 11), offset_vector(key, 5))


def draw_values(key, part):
    return channel_draw(jax.random.fold_in(key, 23), offset_vector(key, 7))


def strengthened(array, own_key, source, target, parts, factor):
    owner, partner = [(jnp.arange(array.shape[position]) // (array.shape[position] // parts)).reshape([-1 if axis == position else 1 for axis in range(array.ndim)]) for position in (source, target)]
    chosen = jax.random.permutation(own_key, parts)[partner]
    strong = (owner == chosen) | (owner == (partner + parts // 2) % parts)
    return jnp.where(strong, factor * array, array)


def block_scale(stream_key, shape, cuts, least, largest):
    loudness, own = 1.0, jax.random.fold_in(stream_key, 6)
    for dim, blocks in cuts:
        steps = jnp.exp(jax.random.uniform(jax.random.fold_in(own, dim), (blocks,), jnp.float32, least / len(cuts), largest / len(cuts)))
        loudness = loudness * jnp.repeat(steps, shape[dim] // blocks).reshape([-1 if axis == dim else 1 for axis in range(len(shape))])
    return loudness


def gaussian(key, extent, spread, limit, cuts=(), kind=jnp.bfloat16):
    entries = spread * jax.random.normal(key, extent, jnp.float32)
    if cuts:
        entries = entries * block_scale(key, extent, cuts, -0.22, 0.18)
    return jnp.clip(entries, -limit, limit).astype(kind)


def bell_draw_with(key, dims, deviation, reach, shards, heavy, kind=jnp.bfloat16):
    values = deviation * jax.random.normal(key, dims, jnp.float32)
    if shards:
        values = values * block_scale(key, dims, shards, -0.22, 0.18)
    return jnp.clip(strengthened(values, jax.random.fold_in(key, 3), *heavy), -reach, reach).astype(kind)


def setup_inputs(seed: int = 0) -> dict:
    seeds = jax.random.split(jax.random.key(seed), 9)
    return {
        "queries": draw_queries(jax.random.fold_in(seeds[8], 71), 0),
        "keys": draw_keys(jax.random.fold_in(seeds[8], 71), 0),
        "values": draw_values(jax.random.fold_in(seeds[8], 71), 0),
        "token_rate": jnp.clip(jnp.exp(math.log(1.0) - 2.9957323 * jax.random.uniform(seeds[3], (TOKENS, HEADS), jnp.float32) ** block_scale(seeds[3], (TOKENS, HEADS), ((0, 32), (1, 4)), -0.2, 0.2)), 0.05, 1.0),
        "head_rate": jnp.clip(jnp.exp(math.log(1.0) - 1.609438 * jax.random.uniform(seeds[4], (HEADS,), jnp.float32) ** block_scale(seeds[4], (HEADS,), ((0, 4),), -0.2, 0.2)), 0.2, 1.0),
        "w_gate": gaussian(seeds[5], (HEADS, DH, FH), DH ** -0.5, 0.25, ((0, 4), (2, 4))),
        "w_up": gaussian(seeds[6], (HEADS, DH, FH), DH ** -0.5, 0.25, ((0, 4), (2, 4))),
        "w_down": bell_draw_with(seeds[7], (HEADS, FH, DH), FH ** -0.5, 0.25, ((0, 4), (1, 4)), (1, 2, 4, 2.0)),
    }


poly_a = 3.4445
poly_b = -4.775
poly_c = 2.0315

def newton_schulz(iterate):
    for sweep_index in range(NS_ITERS):
        gram_full = jnp.dot(iterate, iterate.T, preferred_element_type=jnp.float32).astype(jnp.bfloat16)
        product = jnp.dot(gram_full, iterate, preferred_element_type=jnp.float32).astype(jnp.bfloat16)
        second = jnp.dot(gram_full, product, preferred_element_type=jnp.float32)
        iterate = (poly_a * iterate.astype(jnp.float32) + poly_b * product.astype(jnp.float32) + poly_c * second).astype(jnp.bfloat16)
    return iterate

def orthogonal(gradient):
    norm_value = jnp.sqrt(jnp.sum(gradient * gradient))
    return newton_schulz((gradient / (norm_value + 1e-07)).astype(jnp.bfloat16))

def rescale(fresh, previous, which_dim):
    old_norm = jnp.sqrt(lax.optimization_barrier(jnp.sum(jnp.square(previous.astype(jnp.float32)), axis=which_dim, keepdims=True)))
    new_norm = jnp.sqrt(lax.optimization_barrier(jnp.sum(fresh * fresh, axis=which_dim, keepdims=True)) + 1e-06)
    return (fresh * old_norm / new_norm).astype(jnp.bfloat16)

def one_head(query_part, key_part, value_part, rate_col, step_rate, gate_weight, up_weight, down_weight):
    gate_pre = jnp.dot(key_part, gate_weight, preferred_element_type=jnp.float32)
    up_pre = jnp.dot(key_part, up_weight, preferred_element_type=jnp.float32)
    gate_sig = jax.nn.sigmoid(gate_pre)
    active = gate_pre * gate_sig
    hidden_keys = (active * up_pre).astype(jnp.bfloat16)
    target = (-(rate_col[:, None] * value_part.astype(jnp.float32))).astype(jnp.bfloat16)
    back_hidden = jnp.dot(target, down_weight.T, preferred_element_type=jnp.float32)
    grad_gate = (back_hidden * up_pre * gate_sig * (1.0 + gate_pre * (1.0 - gate_sig))).astype(jnp.bfloat16)
    grad_up = (back_hidden * active).astype(jnp.bfloat16)
    term_gate = jnp.dot(key_part.T, grad_gate, preferred_element_type=jnp.float32)
    term_up = jnp.dot(key_part.T, grad_up, preferred_element_type=jnp.float32)
    term_down = jnp.dot(target.T, hidden_keys, preferred_element_type=jnp.float32)
    ortho_gate = orthogonal(term_gate)
    ortho_up = orthogonal(term_up)
    ortho_down = orthogonal(term_down)
    gate_new = rescale(gate_weight.astype(jnp.float32) - step_rate * ortho_gate.astype(jnp.float32), gate_weight, 0)
    up_new = rescale(up_weight.astype(jnp.float32) - step_rate * ortho_up.astype(jnp.float32), up_weight, 0)
    down_new = rescale(down_weight.astype(jnp.float32) - step_rate * ortho_down.T.astype(jnp.float32), down_weight, 1)
    query_gate = jnp.dot(query_part, gate_new, preferred_element_type=jnp.float32)
    query_up = jnp.dot(query_part, up_new, preferred_element_type=jnp.float32)
    query_hidden = (jax.nn.silu(query_gate) * query_up).astype(jnp.bfloat16)
    block_units = FH // N_HID
    pieces = jnp.einsum('tbf,bfd->btd', query_hidden.reshape(-1, N_HID, block_units).astype(jnp.float32), down_new.reshape(N_HID, block_units, DH).astype(jnp.float32))
    rounded = lax.optimization_barrier(pieces.astype(jnp.bfloat16))
    return lax.optimization_barrier(jnp.sum(rounded.astype(jnp.float32), axis=0)).astype(jnp.bfloat16)

def reference(queries, keys, values, token_rate, head_rate, w_gate, w_up, w_down):
    outputs = []
    for head_index in range(HEADS):
        low_col = head_index * DH
        outputs.append(one_head(queries[:, low_col:low_col + DH], keys[:, low_col:low_col + DH], values[:, low_col:low_col + DH], token_rate[:, head_index], head_rate[head_index], w_gate[head_index], w_up[head_index], w_down[head_index]))
    return jnp.concatenate(outputs, axis=1)
```

```python
import jax
import jax.numpy as jnp
from jax import lax
from jax.sharding import Mesh
from jax.sharding import PartitionSpec as P

NS_ITERS = 3
FAR = 4
NEAR = 4
TOK = ("far", "near", "core")

poly_a = 3.4445
poly_b = -4.775
poly_c = 2.0315


def dot32(left, right, contract):
    return lax.dot_general(left, right, (contract, ((), ())), preferred_element_type=jnp.float32)


def sum_of_copies(pieces, axis):
    got = lax.all_to_all(pieces, axis, 0, 0, tiled=True)
    return jnp.sum(got.astype(jnp.float32), axis=0)


def copies_from(shard, axis):
    size = lax.axis_size(axis)
    return lax.all_to_all(
        jnp.broadcast_to(shard[None], (size, *shard.shape)), axis, 0, 0, tiled=True
    )


def head_gradients(keys, values, rate, gate, up, down):
    gate_pre = dot32(keys, gate, ((1,), (0,)))
    up_pre = dot32(keys, up, ((1,), (0,)))
    gate_sig = jax.nn.sigmoid(gate_pre)
    active = gate_pre * gate_sig
    hidden_keys = (active * up_pre).astype(jnp.bfloat16)
    target = (-(rate * values.astype(jnp.float32))).astype(jnp.bfloat16)
    back_hidden = dot32(target, down, ((1,), (1,)))
    grad_gate = (back_hidden * up_pre * gate_sig * (1.0 + gate_pre * (1.0 - gate_sig))).astype(
        jnp.bfloat16
    )
    grad_up = (back_hidden * active).astype(jnp.bfloat16)
    return jnp.stack(
        (
            dot32(keys, grad_gate, ((0,), (0,))),
            dot32(keys, grad_up, ((0,), (0,))),
            dot32(target, hidden_keys, ((0,), (0,))),
        )
    )


def newton_schulz(blocks, own):
    sq_norm = jnp.sum(jnp.square(blocks.astype(jnp.float32)))
    scale = 1.0 / (jnp.sqrt(sq_norm) + 1e-07)
    current = blocks
    for iteration in range(NS_ITERS):
        first = scale if iteration == 0 else None
        gram = jnp.einsum("xrf,xcf->rc", current, current, preferred_element_type=jnp.float32)
        if first is not None:
            gram = gram * (first * first)
        gram = gram.astype(jnp.bfloat16)
        if iteration == NS_ITERS - 1:
            current = lax.dynamic_slice_in_dim(current, own, 1, 0)
        product = jnp.einsum("rc,xcf->xrf", gram, current, preferred_element_type=jnp.float32)
        if first is not None:
            product = product * first
        product = product.astype(jnp.bfloat16)
        second = jnp.einsum("rc,xcf->xrf", gram, product, preferred_element_type=jnp.float32)
        leading = current.astype(jnp.float32)
        if first is not None:
            leading = leading * first
        current = (
            poly_a * leading + poly_b * product.astype(jnp.float32) + poly_c * second
        ).astype(jnp.bfloat16)
    return current[0]


def rescale(fresh, previous):
    old_norm = jnp.sqrt(jnp.sum(jnp.square(previous), axis=0, keepdims=True))
    new_norm = jnp.sqrt(jnp.sum(fresh * fresh, axis=0, keepdims=True) + 1e-06)
    return (fresh * old_norm / new_norm).astype(jnp.bfloat16)


def local(queries, keys, values, token_rate, head_rate, w_gate, w_up, w_down):
    tok_rows, all_cols = keys.shape
    heads_here = token_rate.shape[1]
    width = all_cols // heads_here
    units = w_gate.shape[2]
    chunk = width // NEAR
    core = lax.axis_index("core")
    slot = lax.axis_index("far")
    near = lax.axis_index("near")
    hid = lax.axis_index("hid")
    other = 1 - core

    def gradients_of(head):
        cols = head * width
        return head_gradients(
            lax.dynamic_slice_in_dim(keys, cols, width, 1),
            lax.dynamic_slice_in_dim(values, cols, width, 1),
            lax.dynamic_slice_in_dim(token_rate, head, 1, 1),
            lax.dynamic_index_in_dim(w_gate, head, 0, False),
            lax.dynamic_index_in_dim(w_up, head, 0, False),
            lax.dynamic_index_in_dim(w_down, head, 0, False),
        )

    swap = [(0, 1), (1, 0)]
    received = lax.ppermute(gradients_of(other).astype(jnp.bfloat16), "core", swap)
    summed = gradients_of(core) + received.astype(jnp.float32)
    pieces = summed.astype(jnp.bfloat16).reshape(3, NEAR, chunk, units).swapaxes(0, 1)
    near_sum = sum_of_copies(pieces, "near").astype(jnp.bfloat16)
    slots = jnp.concatenate((near_sum, near_sum[:1]), axis=0)
    total = sum_of_copies(slots, "far").astype(jnp.bfloat16)
    rows = lax.all_gather(total, "near", axis=0, tiled=True)
    blocks = copies_from(rows, "hid")
    ortho = newton_schulz(blocks, hid).astype(jnp.float32)

    old = lax.switch(
        jnp.minimum(slot, 2),
        (
            lambda: lax.dynamic_index_in_dim(w_gate, core, 0, False),
            lambda: lax.dynamic_index_in_dim(w_up, core, 0, False),
            lambda: lax.dynamic_index_in_dim(w_down, core, 0, False).T,
        ),
    ).astype(jnp.float32)
    fresh = old - lax.dynamic_index_in_dim(head_rate, core, 0, False) * ortho
    renewed = rescale(fresh, old)
    share = lax.dynamic_slice_in_dim(renewed, near * chunk, chunk, 0)
    by_slot = lax.all_gather(share, "far", axis=0)[:3]
    mine = lax.all_gather(by_slot, "near", axis=1).reshape(3, width, units)
    both = lax.all_gather(mine, "core", axis=0)

    terms = []
    for head in range(heads_here):
        query_rows = queries[:, head * width : (head + 1) * width]
        query_gate = dot32(query_rows, both[head, 0], ((1,), (0,)))
        query_up = dot32(query_rows, both[head, 1], ((1,), (0,)))
        query_hidden = (jax.nn.silu(query_gate) * query_up).astype(jnp.bfloat16)
        term = dot32(query_hidden, both[head, 2], ((1,), (1,))).astype(jnp.bfloat16)
        for half in range(2):
            terms.append(term[:, half * (width // 2) : (half + 1) * (width // 2)])
    return sum_of_copies(jnp.stack(terms), "hid").astype(jnp.bfloat16)


def solution(mesh):
    finer = Mesh(
        mesh.devices.reshape(mesh.shape["head"], FAR, NEAR, 2, mesh.shape["hid"]),
        ("head", "far", "near", "core", "hid"),
    )
    return jax.shard_map(
        local,
        mesh=finer,
        in_specs=(
            P(TOK, "head"),
            P(TOK, "head"),
            P(TOK, "head"),
            P(TOK, "head"),
            P("head"),
            P("head", None, "hid"),
            P("head", None, "hid"),
            P("head", "hid", None),
        ),
        out_specs=P(TOK, ("head", "hid")),
        check_vma=False,
    )
```

```python
import jax
import jax.numpy as jnp
from jax import lax
from jax.sharding import Mesh
from jax.sharding import PartitionSpec as P

NS_ITERS = 3
TOK = ("z", "core")

poly_a = 3.4445
poly_b = -4.775
poly_c = 2.0315


def dot32(left, right, contract):
    return lax.dot_general(left, right, (contract, ((), ())), preferred_element_type=jnp.float32)


def sum_of_copies(pieces, axis):
    got = lax.all_to_all(pieces, axis, 0, 0, tiled=True)
    return jnp.sum(got.astype(jnp.float32), axis=0)


def head_gradients(keys, values, rate, gate, up, down):
    gate_pre = dot32(keys, gate, ((1,), (0,)))
    up_pre = dot32(keys, up, ((1,), (0,)))
    gate_sig = jax.nn.sigmoid(gate_pre)
    active = gate_pre * gate_sig
    hidden_keys = (active * up_pre).astype(jnp.bfloat16)
    target = (-(rate * values.astype(jnp.float32))).astype(jnp.bfloat16)
    back_hidden = dot32(target, down, ((1,), (1,)))
    grad_gate = (back_hidden * up_pre * gate_sig * (1.0 + gate_pre * (1.0 - gate_sig))).astype(
        jnp.bfloat16
    )
    grad_up = (back_hidden * active).astype(jnp.bfloat16)
    return jnp.stack(
        (
            dot32(keys, grad_gate, ((0,), (0,))),
            dot32(keys, grad_up, ((0,), (0,))),
            dot32(target, hidden_keys, ((0,), (0,))),
        )
    )


def newton_schulz(blocks):
    sq_norm = jnp.sum(jnp.square(blocks.astype(jnp.float32)))
    scale = 1.0 / (jnp.sqrt(sq_norm) + 1e-07)
    current = blocks
    for iteration in range(NS_ITERS):
        factor = scale if iteration == 0 else 1.0
        gram = jnp.einsum("xrf,xcf->rc", current, current, preferred_element_type=jnp.float32)
        gram = (gram * (factor * factor)).astype(jnp.bfloat16)
        product = jnp.einsum("rc,xcf->xrf", gram, current, preferred_element_type=jnp.float32)
        product = (product * factor).astype(jnp.bfloat16)
        second = jnp.einsum("rc,xcf->xrf", gram, product, preferred_element_type=jnp.float32)
        current = (
            poly_a * (factor * current.astype(jnp.float32))
            + poly_b * product.astype(jnp.float32)
            + poly_c * second
        ).astype(jnp.bfloat16)
    return current


def rescale(fresh, previous):
    old_norm = jnp.sqrt(jnp.sum(jnp.square(previous), axis=1, keepdims=True))
    new_norm = jnp.sqrt(jnp.sum(fresh * fresh, axis=1, keepdims=True) + 1e-06)
    return (fresh * old_norm / new_norm).astype(jnp.bfloat16)


def local(queries, keys, values, token_rate, head_rate, w_gate, w_up, w_down):
    tok_rows, all_cols = keys.shape
    width = all_cols // token_rate.shape[1]
    units = w_gate.shape[2]
    chunk = width // lax.axis_size("z")
    core = lax.axis_index("core")
    other = 1 - core

    def gradients_of(head):
        cols = head * width
        return head_gradients(
            lax.dynamic_slice_in_dim(keys, cols, width, 1),
            lax.dynamic_slice_in_dim(values, cols, width, 1),
            lax.dynamic_slice_in_dim(token_rate, head, 1, 1),
            lax.dynamic_index_in_dim(w_gate, head, 0, False),
            lax.dynamic_index_in_dim(w_up, head, 0, False),
            lax.dynamic_index_in_dim(w_down, head, 0, False),
        )

    swap = [(0, 1), (1, 0)]
    received = lax.ppermute(gradients_of(other).astype(jnp.bfloat16), "core", swap)
    summed = gradients_of(core) + received.astype(jnp.float32)
    pieces = summed.astype(jnp.bfloat16).reshape(3, -1, chunk, units).swapaxes(0, 1)
    owned = sum_of_copies(pieces, "z").astype(jnp.bfloat16)
    full = lax.all_gather(owned, "z", axis=1, tiled=True)
    blocks = lax.all_to_all(jnp.concatenate((full, full[:1]), axis=0), "hid", 0, 0, tiled=True)
    ortho = lax.all_to_all(newton_schulz(blocks), "hid", 0, 0, tiled=True)[:3]

    old = jnp.stack(
        (
            lax.dynamic_index_in_dim(w_gate, core, 0, False),
            lax.dynamic_index_in_dim(w_up, core, 0, False),
            lax.dynamic_index_in_dim(w_down, core, 0, False).T,
        )
    ).astype(jnp.float32)
    step = lax.dynamic_index_in_dim(head_rate, core, 0, False)
    mine = rescale(old - step * ortho.astype(jnp.float32), old)
    theirs = lax.ppermute(mine, "core", swap)

    def term_of(head, weights):
        rows = lax.dynamic_slice_in_dim(queries, head * width, width, 1)
        query_gate = dot32(rows, weights[0], ((1,), (0,)))
        query_up = dot32(rows, weights[1], ((1,), (0,)))
        query_hidden = (jax.nn.silu(query_gate) * query_up).astype(jnp.bfloat16)
        halves = [
            dot32(query_hidden, weights[2][part], ((1,), (1,))).astype(jnp.bfloat16)
            for part in (slice(0, width // 2), slice(width // 2, width))
        ]
        return jnp.stack(halves)

    own_term = term_of(core, mine)
    other_term = term_of(other, theirs)
    is_first = core == 0
    terms = jnp.concatenate(
        (
            jnp.where(is_first, own_term, other_term),
            jnp.where(is_first, other_term, own_term),
        )
    )
    return sum_of_copies(terms, "hid").astype(jnp.bfloat16)


def solution(mesh):
    finer = Mesh(
        mesh.devices.reshape(mesh.shape["head"], -1, 2, mesh.shape["hid"]),
        ("head", "z", "core", "hid"),
    )
    return jax.shard_map(
        local,
        mesh=finer,
        in_specs=(
            P(TOK, "head"),
            P(TOK, "head"),
            P(TOK, "head"),
            P(TOK, "head"),
            P("head"),
            P("head", None, "hid"),
            P("head", None, "hid"),
            P("head", "hid", None),
        ),
        out_specs=P(TOK, ("head", "hid")),
        check_vma=False,
    )
```

```python
import jax
import jax.numpy as jnp
from jax import lax
from jax.sharding import Mesh
from jax.sharding import PartitionSpec as P

NS_ITERS = 3
Z = ("pair", "parity")
TOK = ("pair", "parity", "core")

poly_a = 3.4445
poly_b = -4.775
poly_c = 2.0315


def dot32(left, right, contract):
    return lax.dot_general(left, right, (contract, ((), ())), preferred_element_type=jnp.float32)


def sum_of_copies(pieces, axis):
    got = lax.all_to_all(pieces, axis, 0, 0, tiled=True)
    return jnp.sum(got.astype(jnp.float32), axis=0)


def halves_by_parity(blocks, odd, dim):
    def quarter(index):
        return lax.dynamic_index_in_dim(blocks, index, dim, False)

    kept = [quarter(2 * part + odd) for part in range(2)]
    sent = [quarter(2 * part + 1 - odd) for part in range(2)]
    return kept, sent


def head_gradients(keys, values, rate, gate, up, down):
    gate_pre = dot32(keys, gate, ((1,), (0,)))
    up_pre = dot32(keys, up, ((1,), (0,)))
    gate_sig = jax.nn.sigmoid(gate_pre)
    active = gate_pre * gate_sig
    hidden_keys = (active * up_pre).astype(jnp.bfloat16)
    target = (-(rate * values.astype(jnp.float32))).astype(jnp.bfloat16)
    back_hidden = dot32(target, down, ((1,), (1,)))
    grad_gate = (back_hidden * up_pre * gate_sig * (1.0 + gate_pre * (1.0 - gate_sig))).astype(
        jnp.bfloat16
    )
    grad_up = (back_hidden * active).astype(jnp.bfloat16)
    return jnp.stack(
        (
            dot32(keys, grad_gate, ((0,), (0,))),
            dot32(keys, grad_up, ((0,), (0,))),
            dot32(target, hidden_keys, ((0,), (0,))),
        )
    )


def newton_schulz(blocks):
    sq_norm = jnp.sum(jnp.square(blocks.astype(jnp.float32)))
    scale = 1.0 / (jnp.sqrt(sq_norm) + 1e-07)
    current = blocks
    for iteration in range(NS_ITERS):
        factor = scale if iteration == 0 else 1.0
        gram = jnp.einsum("xrf,xcf->rc", current, current, preferred_element_type=jnp.float32)
        gram = (gram * (factor * factor)).astype(jnp.bfloat16)
        product = jnp.einsum("rc,xcf->xrf", gram, current, preferred_element_type=jnp.float32)
        product = (product * factor).astype(jnp.bfloat16)
        second = jnp.einsum("rc,xcf->xrf", gram, product, preferred_element_type=jnp.float32)
        current = (
            poly_a * (factor * current.astype(jnp.float32))
            + poly_b * product.astype(jnp.float32)
            + poly_c * second
        ).astype(jnp.bfloat16)
    return current


def rescale(fresh, previous):
    old_norm = jnp.sqrt(jnp.sum(jnp.square(previous), axis=1, keepdims=True))
    new_norm = jnp.sqrt(jnp.sum(fresh * fresh, axis=1, keepdims=True) + 1e-06)
    return (fresh * old_norm / new_norm).astype(jnp.bfloat16)


def local(queries, keys, values, token_rate, head_rate, w_gate, w_up, w_down):
    tok_rows, all_cols = keys.shape
    width = all_cols // token_rate.shape[1]
    units = w_gate.shape[2]
    chunk = width // lax.axis_size(Z)
    odd = lax.axis_index("parity")
    depth = lax.axis_size(Z)
    ways = (
        [(at, at ^ 1) for at in range(depth)],
        [(at, (at + (1 if at % 2 else -1)) % depth) for at in range(depth)],
    )
    core = lax.axis_index("core")
    other = 1 - core

    def gradients_of(head):
        cols = head * width
        return head_gradients(
            lax.dynamic_slice_in_dim(keys, cols, width, 1),
            lax.dynamic_slice_in_dim(values, cols, width, 1),
            lax.dynamic_slice_in_dim(token_rate, head, 1, 1),
            lax.dynamic_index_in_dim(w_gate, head, 0, False),
            lax.dynamic_index_in_dim(w_up, head, 0, False),
            lax.dynamic_index_in_dim(w_down, head, 0, False),
        )

    swap = [(0, 1), (1, 0)]
    received = lax.ppermute(gradients_of(other).astype(jnp.bfloat16), "core", swap)
    summed = gradients_of(core) + received.astype(jnp.float32)
    summed = summed.astype(jnp.bfloat16).reshape(3, 4, width // 4, units)
    kept, sent = halves_by_parity(summed, odd, 1)
    pair_sum = jnp.stack(
        [
            kept[part].astype(jnp.float32)
            + lax.ppermute(sent[part], Z, ways[part]).astype(jnp.float32)
            for part in range(2)
        ],
        axis=1,
    ).astype(jnp.bfloat16)
    pieces = pair_sum.reshape(3, -1, chunk, units).swapaxes(0, 1)
    owned = sum_of_copies(pieces, "pair").astype(jnp.bfloat16)
    held = lax.all_gather(owned, "pair", axis=1, tiled=True).reshape(3, 2, width // 4, units)
    brought = [lax.ppermute(held[:, part], Z, ways[part]) for part in range(2)]
    full = jnp.stack(
        [
            jnp.where(odd == place, held[:, part], brought[part])
            for part in range(2)
            for place in range(2)
        ],
        axis=1,
    ).reshape(3, width, units)
    blocks = lax.all_to_all(jnp.concatenate((full, full[:1]), axis=0), "hid", 0, 0, tiled=True)
    ortho = lax.all_to_all(newton_schulz(blocks), "hid", 0, 0, tiled=True)[:3]

    old = jnp.stack(
        (
            lax.dynamic_index_in_dim(w_gate, core, 0, False),
            lax.dynamic_index_in_dim(w_up, core, 0, False),
            lax.dynamic_index_in_dim(w_down, core, 0, False).T,
        )
    ).astype(jnp.float32)
    step = lax.dynamic_index_in_dim(head_rate, core, 0, False)
    mine = rescale(old - step * ortho.astype(jnp.float32), old)
    theirs = lax.ppermute(mine, "core", swap)

    def term_of(head, weights):
        rows = lax.dynamic_slice_in_dim(queries, head * width, width, 1)
        query_gate = dot32(rows, weights[0], ((1,), (0,)))
        query_up = dot32(rows, weights[1], ((1,), (0,)))
        query_hidden = (jax.nn.silu(query_gate) * query_up).astype(jnp.bfloat16)
        halves = [
            dot32(query_hidden, weights[2][part], ((1,), (1,))).astype(jnp.bfloat16)
            for part in (slice(0, width // 2), slice(width // 2, width))
        ]
        return jnp.stack(halves)

    own_term = term_of(core, mine)
    other_term = term_of(other, theirs)
    is_first = core == 0
    terms = jnp.concatenate(
        (
            jnp.where(is_first, own_term, other_term),
            jnp.where(is_first, other_term, own_term),
        )
    )
    return sum_of_copies(terms, "hid").astype(jnp.bfloat16)


def solution(mesh):
    finer = Mesh(
        mesh.devices.reshape(mesh.shape["head"], -1, 2, 2, mesh.shape["hid"]),
        ("head", "pair", "parity", "core", "hid"),
    )
    return jax.shard_map(
        local,
        mesh=finer,
        in_specs=(
            P(TOK, "head"),
            P(TOK, "head"),
            P(TOK, "head"),
            P(TOK, "head"),
            P("head"),
            P("head", None, "hid"),
            P("head", None, "hid"),
            P("head", "hid", None),
        ),
        out_specs=P(TOK, ("head", "hid")),
        check_vma=False,
    )
```

```python
import jax
import jax.numpy as jnp
from jax import lax
from jax.experimental import pallas as pl
from jax.experimental.pallas import tpu as pltpu
from jax.sharding import Mesh
from jax.sharding import PartitionSpec as P

NS_ITERS = 3
TOK = ("z", "core")
KINDS = 3
TILE = 128

poly_a = 3.4445
poly_b = -4.775
poly_c = 2.0315


def dot32(left, right, contract):
    return lax.dot_general(left, right, (contract, ((), ())), preferred_element_type=jnp.float32)


def sum_of_copies(pieces, axis):
    got = lax.all_to_all(pieces, axis, 0, 0, tiled=True)
    return jnp.sum(got.astype(jnp.float32), axis=0)


def sigmoid(value):
    return 1.0 / (1.0 + jnp.exp(-value))


def gradients_kernel(head_ref, keys, values, rate, gate, up, down, out, target, d_gate, d_up, hidden):
    first = head_ref[0] == 0
    rows = keys.shape[0]
    for start in range(0, rows, TILE):
        part = slice(start, start + TILE)
        own_rate = jnp.where(first, rate[part, 0:1], rate[part, 1:2])
        goal = (-(own_rate * values[part, :].astype(jnp.float32))).astype(jnp.bfloat16)
        target[part, :] = goal
        gate_pre = dot32(keys[part, :], gate[0], ((1,), (0,)))
        up_pre = dot32(keys[part, :], up[0], ((1,), (0,)))
        back = dot32(goal, down[0], ((1,), (1,)))
        gate_sig = sigmoid(gate_pre)
        active = gate_pre * gate_sig
        hidden[part, :] = (active * up_pre).astype(jnp.bfloat16)
        d_gate[part, :] = (back * up_pre * gate_sig * (1.0 + gate_pre * (1.0 - gate_sig))).astype(
            jnp.bfloat16
        )
        d_up[part, :] = (back * active).astype(jnp.bfloat16)
    depth, _, chunk, units = out.shape
    for kind, (left, right) in enumerate(((keys, d_gate), (keys, d_up), (target, hidden))):
        term = dot32(left[...], right[...], ((0,), (0,))).astype(jnp.bfloat16)
        out[:, kind] = term.reshape(depth, chunk, units)


def newton_schulz_kernel(blocks, out, iterate, product, gram, raw):
    count, rows, units = blocks.shape
    columns = [slice(at * units, (at + 1) * units) for at in range(count)]
    halves = [slice(at, at + units) for at in range(0, rows, units)]
    for at in range(count):
        iterate[:, columns[at]] = blocks[at]
    scale = None
    for iteration in range(NS_ITERS):
        if iteration == 0:
            trace = jnp.zeros((1, 1), jnp.float32)
            for half in halves:
                block = dot32(iterate[...], iterate[half, :], ((1,), (1,)))
                raw[:, half] = block
                square = block[half, :]
                line = lax.broadcasted_iota(jnp.int32, square.shape, 0)
                column = lax.broadcasted_iota(jnp.int32, square.shape, 1)
                trace = trace + jnp.sum(
                    jnp.where(line == column, square, 0.0), axis=(0, 1), keepdims=True
                )
            scale = 1.0 / (jnp.sqrt(trace) + 1e-07)
            for half in halves:
                gram[:, half] = (raw[:, half] * (scale * scale)).astype(jnp.bfloat16)
        else:
            for half in halves:
                gram[:, half] = dot32(iterate[...], iterate[half, :], ((1,), (1,))).astype(
                    jnp.bfloat16
                )
        for at in range(count):
            block = dot32(gram[...], iterate[:, columns[at]], ((1,), (0,)))
            if iteration == 0:
                block = block * scale
            product[:, columns[at]] = block.astype(jnp.bfloat16)
        for at in range(count):
            second = dot32(gram[...], product[:, columns[at]], ((1,), (0,)))
            leading = iterate[:, columns[at]].astype(jnp.float32)
            if iteration == 0:
                leading = leading * scale
            block = (
                poly_a * leading
                + poly_b * product[:, columns[at]].astype(jnp.float32)
                + poly_c * second
            ).astype(jnp.bfloat16)
            if iteration == NS_ITERS - 1:
                out[at] = block
            else:
                iterate[:, columns[at]] = block


def rescale_kernel(head_ref, head_rate, ortho, gate, up, down, out):
    step = head_rate[head_ref[0]]
    for kind in range(KINDS):
        if kind == 2:
            old = down[0].astype(jnp.float32).T
        else:
            old = (gate, up)[kind][0].astype(jnp.float32)
        fresh = old - step * ortho[kind].astype(jnp.float32)
        old_norm = jnp.sqrt(jnp.sum(old * old, axis=0, keepdims=True))
        new_norm = jnp.sqrt(jnp.sum(fresh * fresh, axis=0, keepdims=True) + 1e-06)
        out[kind] = (fresh * (old_norm / new_norm)).astype(jnp.bfloat16)


def query_kernel(head_ref, queries, weights, *rest):
    out = rest[-1]
    half = out.shape[2]
    rows = queries.shape[0]
    for start in range(0, rows, 2 * TILE):
        part = slice(start, start + 2 * TILE)
        query_gate = dot32(queries[part, :], weights[0], ((1,), (0,)))
        query_up = dot32(queries[part, :], weights[1], ((1,), (0,)))
        query_hidden = (query_gate * sigmoid(query_gate) * query_up).astype(jnp.bfloat16)
        for at in range(out.shape[0]):
            features = weights[2, at * half : (at + 1) * half, :]
            out[at, part, :] = dot32(query_hidden, features, ((1,), (1,))).astype(jnp.bfloat16)


def cost(flops, operands):
    return pl.CostEstimate(flops=flops, transcendentals=0, bytes_accessed=operands)


def gradients_of(head, keys, values, rate, gate, up, down, depth):
    rows, width = keys.shape[0], gate.shape[1]
    units = gate.shape[2]
    columns = pl.BlockSpec((rows, width), lambda step, head: (0, head[0]))
    weight = pl.BlockSpec((1, width, units), lambda step, head: (head[0], 0, 0))
    return pl.pallas_call(
        gradients_kernel,
        grid_spec=pltpu.PrefetchScalarGridSpec(
            num_scalar_prefetch=1,
            grid=(1,),
            in_specs=[
                columns,
                columns,
                pl.BlockSpec(rate.shape, lambda step, head: (0, 0)),
                weight,
                weight,
                pl.BlockSpec((1, units, width), lambda step, head: (head[0], 0, 0)),
            ],
            out_specs=pl.BlockSpec(
                (depth, KINDS, width // depth, units), lambda step, head: (0, 0, 0, 0)
            ),
            scratch_shapes=[
                pltpu.VMEM((rows, width), jnp.bfloat16),
                pltpu.VMEM((rows, units), jnp.bfloat16),
                pltpu.VMEM((rows, units), jnp.bfloat16),
                pltpu.VMEM((rows, units), jnp.bfloat16),
            ],
        ),
        out_shape=jax.ShapeDtypeStruct((depth, KINDS, width // depth, units), jnp.bfloat16),
        cost_estimate=cost(12 * rows * width * units, 4 * rows * width),
        name="gradients",
    )(head, keys, values, rate, gate, up, down)


def newton_schulz(blocks):
    count, rows, units = blocks.shape
    return pl.pallas_call(
        newton_schulz_kernel,
        out_shape=jax.ShapeDtypeStruct(blocks.shape, blocks.dtype),
        scratch_shapes=[
            pltpu.VMEM((rows, count * units), jnp.bfloat16),
            pltpu.VMEM((rows, count * units), jnp.bfloat16),
            pltpu.VMEM((rows, rows), jnp.bfloat16),
            pltpu.VMEM((rows, rows), jnp.float32),
        ],
        cost_estimate=cost(18 * rows * rows * count * units, 4 * blocks.size),
        name="newton_schulz",
    )(blocks)


def rescaled(head, head_rate, ortho, gate, up, down):
    _, width, units = gate.shape
    weight = pl.BlockSpec((1, width, units), lambda step, head: (head[0], 0, 0))
    return pl.pallas_call(
        rescale_kernel,
        grid_spec=pltpu.PrefetchScalarGridSpec(
            num_scalar_prefetch=1,
            grid=(1,),
            in_specs=[
                pl.BlockSpec(memory_space=pltpu.SMEM),
                pl.BlockSpec((KINDS, width, units), lambda step, head: (0, 0, 0)),
                weight,
                weight,
                pl.BlockSpec((1, units, width), lambda step, head: (head[0], 0, 0)),
            ],
            out_specs=pl.BlockSpec((KINDS, width, units), lambda step, head: (0, 0, 0)),
        ),
        out_shape=jax.ShapeDtypeStruct((KINDS, width, units), jnp.bfloat16),
        cost_estimate=cost(20 * KINDS * width * units, 6 * KINDS * width * units),
        name="rescale",
    )(head, head_rate, ortho, gate, up, down)


def query_terms(head, queries, weights, earlier=None):
    rows = queries.shape[0]
    _, width, units = weights.shape
    pieces = width // units
    shape = jax.ShapeDtypeStruct((2 * pieces, rows, units), jnp.bfloat16)
    return pl.pallas_call(
        query_kernel,
        grid_spec=pltpu.PrefetchScalarGridSpec(
            num_scalar_prefetch=1,
            grid=(1,),
            in_specs=[
                pl.BlockSpec((rows, width), lambda step, head: (0, head[0])),
                pl.BlockSpec(weights.shape, lambda step, head: (0, 0, 0)),
            ]
            + ([] if earlier is None else [pl.BlockSpec(memory_space=pl.ANY)]),
            out_specs=pl.BlockSpec((pieces, rows, units), lambda step, head: (head[0], 0, 0)),
        ),
        out_shape=shape,
        input_output_aliases={} if earlier is None else {3: 0},
        cost_estimate=cost(6 * rows * width * units, 4 * rows * width),
        name="query",
    )(head, queries, weights, *(() if earlier is None else (earlier,)))


def local(queries, keys, values, token_rate, head_rate, w_gate, w_up, w_down):
    core = lax.axis_index("core").astype(jnp.int32)
    mine, theirs = core.reshape(1), (1 - core).reshape(1)
    swap = [(0, 1), (1, 0)]
    given = (keys, values, token_rate, w_gate, w_up, w_down, lax.axis_size("z"))
    received = lax.ppermute(gradients_of(theirs, *given), "core", swap)
    pieces = (
        gradients_of(mine, *given).astype(jnp.float32) + received.astype(jnp.float32)
    ).astype(jnp.bfloat16)
    owned = sum_of_copies(pieces, "z").astype(jnp.bfloat16)
    full = lax.all_gather(owned, "z", axis=1, tiled=True)
    blocks = lax.all_to_all(jnp.concatenate((full, full[:1]), axis=0), "hid", 0, 0, tiled=True)
    ortho = lax.all_to_all(newton_schulz(blocks), "hid", 0, 0, tiled=True)
    new = rescaled(mine, head_rate, ortho, w_gate, w_up, w_down)
    new_there = lax.ppermute(new, "core", swap)
    terms = query_terms(theirs, queries, new_there, query_terms(mine, queries, new))
    return sum_of_copies(terms, "hid").astype(jnp.bfloat16)


def solution(mesh):
    finer = Mesh(
        mesh.devices.reshape(mesh.shape["head"], -1, 2, mesh.shape["hid"]),
        ("head", "z", "core", "hid"),
    )
    return jax.shard_map(
        local,
        mesh=finer,
        in_specs=(
            P(TOK, "head"),
            P(TOK, "head"),
            P(TOK, "head"),
            P(TOK, "head"),
            P("head"),
            P("head", None, "hid"),
            P("head", None, "hid"),
            P("head", "hid", None),
        ),
        out_specs=P(TOK, ("head", "hid")),
        check_vma=False,
    )
```

```python
import jax
import jax.numpy as jnp
from jax import lax
from jax.experimental import pallas as pl
from jax.experimental.pallas import tpu as pltpu
from jax.sharding import Mesh
from jax.sharding import PartitionSpec as P

NS_ITERS = 3
TOK = ("z", "core")
KINDS = 3
TILE = 128

poly_a = 3.4445
poly_b = -4.775
poly_c = 2.0315


def dot32(left, right, contract):
    return lax.dot_general(left, right, (contract, ((), ())), preferred_element_type=jnp.float32)


def sum_of_copies(pieces, axis):
    got = lax.all_to_all(pieces, axis, 0, 0, tiled=True)
    return jnp.sum(got.astype(jnp.float32), axis=0)


def sigmoid(value):
    return 1.0 / (1.0 + jnp.exp(-value))


def head_gradients(head, lines, values, rates, gate, up, down, out, target, d_gate, d_up, hidden):
    first = head == 0
    rows, width = lines.shape
    for start in range(0, rows, TILE):
        part = slice(start, start + TILE)
        rate = jnp.where(first, rates[0:1, part], rates[1:2, part])
        rate = jnp.broadcast_to(rate, (TILE, TILE)).T
        rate = jnp.concatenate([rate] * (width // TILE), axis=1)
        goal = (-(rate * values[part, :].astype(jnp.float32))).astype(jnp.bfloat16)
        target[part, :] = goal
        gate_pre = dot32(lines[part, :], gate[...], ((1,), (0,)))
        up_pre = dot32(lines[part, :], up[...], ((1,), (0,)))
        back = dot32(goal, down[...], ((1,), (1,)))
        gate_sig = sigmoid(gate_pre)
        active = gate_pre * gate_sig
        hidden[part, :] = (active * up_pre).astype(jnp.bfloat16)
        d_gate[part, :] = (back * up_pre * gate_sig * (1.0 + gate_pre * (1.0 - gate_sig))).astype(
            jnp.bfloat16
        )
        d_up[part, :] = (back * active).astype(jnp.bfloat16)
    depth, _, chunk, units = out.shape
    for kind, (left, right) in enumerate(((lines, d_gate), (lines, d_up), (target, hidden))):
        term = dot32(left[...], right[...], ((0,), (0,))).astype(jnp.bfloat16)
        out[:, kind] = term.reshape(depth, chunk, units)


def first_head_kernel(heads, rates, keys, values, gate, up, down, out, *rest):
    kept, held, work, sems = rest[:5], rest[5:10], rest[10:14], rest[14]
    width = held[0].shape[1]
    copies = []
    for turn, places in enumerate((held, kept)):
        head = heads[turn]
        columns = pl.ds(pl.multiple_of(head * width, width), width)
        sources = (keys.at[:, columns], values.at[:, columns], gate.at[head], up.at[head], down.at[head])
        for at, (source, place) in enumerate(zip(sources, places)):
            copy = pltpu.make_async_copy(source, place, sems.at[turn, at])
            copy.start()
            copies.append(copy)
    for copy in copies[:5]:
        copy.wait()
    lines, goals, own_gate, own_up, own_down = held
    head_gradients(heads[0], lines, goals, rates, own_gate, own_up, own_down, out, *work)
    for copy in copies[5:]:
        copy.wait()


def second_head_kernel(head_ref, rates, lines, values, gate, up, down, out, *work):
    head_gradients(head_ref[0], lines, values, rates, gate, up, down, out, *work)


def newton_schulz_kernel(blocks, out, iterate, product, gram, raw):
    count, rows, units = blocks.shape
    columns = [slice(at * units, (at + 1) * units) for at in range(count)]
    halves = [slice(at, at + units) for at in range(0, rows, units)]
    for at in range(count):
        iterate[:, columns[at]] = blocks[at]
    scale = None
    for iteration in range(NS_ITERS):
        if iteration == 0:
            trace = jnp.zeros((1, 1), jnp.float32)
            for half in halves:
                block = dot32(iterate[...], iterate[half, :], ((1,), (1,)))
                raw[:, half] = block
                square = block[half, :]
                line = lax.broadcasted_iota(jnp.int32, square.shape, 0)
                column = lax.broadcasted_iota(jnp.int32, square.shape, 1)
                trace = trace + jnp.sum(
                    jnp.where(line == column, square, 0.0), axis=(0, 1), keepdims=True
                )
            scale = 1.0 / (jnp.sqrt(trace) + 1e-07)
            for half in halves:
                gram[:, half] = (raw[:, half] * (scale * scale)).astype(jnp.bfloat16)
        else:
            for half in halves:
                gram[:, half] = dot32(iterate[...], iterate[half, :], ((1,), (1,))).astype(
                    jnp.bfloat16
                )
        for at in range(count):
            block = dot32(gram[...], iterate[:, columns[at]], ((1,), (0,)))
            if iteration == 0:
                block = block * scale
            product[:, columns[at]] = block.astype(jnp.bfloat16)
        for at in range(count):
            second = dot32(gram[...], product[:, columns[at]], ((1,), (0,)))
            leading = iterate[:, columns[at]].astype(jnp.float32)
            if iteration == 0:
                leading = leading * scale
            block = (
                poly_a * leading
                + poly_b * product[:, columns[at]].astype(jnp.float32)
                + poly_c * second
            ).astype(jnp.bfloat16)
            if iteration == NS_ITERS - 1:
                out[at] = block
            else:
                iterate[:, columns[at]] = block


def rescale_kernel(head_ref, head_rate, ortho, gate, up, down, out):
    step = head_rate[head_ref[0]]
    for kind in range(KINDS):
        if kind == 2:
            old = down[...].astype(jnp.float32).T
        else:
            old = (gate, up)[kind][...].astype(jnp.float32)
        fresh = old - step * ortho[kind].astype(jnp.float32)
        old_norm = jnp.sqrt(jnp.sum(old * old, axis=0, keepdims=True))
        new_norm = jnp.sqrt(jnp.sum(fresh * fresh, axis=0, keepdims=True) + 1e-06)
        out[kind] = (fresh * (old_norm / new_norm)).astype(jnp.bfloat16)


def query_kernel(head_ref, queries, weights, *rest):
    out = rest[-1]
    head = head_ref[0]
    _, width, units = weights.shape
    pieces = width // units
    rows = queries.shape[0]
    columns = pl.ds(pl.multiple_of(head * width, width), width)
    base = 0
    if len(rest) == 2:
        base = head * pieces
        out[pl.ds(pieces - base, pieces)] = rest[0][...]
    for start in range(0, rows, 2 * TILE):
        part = slice(start, start + 2 * TILE)
        lines = queries[part, columns]
        query_gate = dot32(lines, weights[0], ((1,), (0,)))
        query_up = dot32(lines, weights[1], ((1,), (0,)))
        query_hidden = (query_gate * sigmoid(query_gate) * query_up).astype(jnp.bfloat16)
        for at in range(pieces):
            features = weights[2, at * units : (at + 1) * units, :]
            out[base + at, part, :] = dot32(query_hidden, features, ((1,), (1,))).astype(
                jnp.bfloat16
            )


def cost(flops, operands):
    return pl.CostEstimate(flops=flops, transcendentals=0, bytes_accessed=operands)


def in_vmem(kernel, name, out_shape, scalars, operands, scratch, flops, far=()):
    near = pl.BlockSpec(memory_space=pltpu.VMEM)
    several = isinstance(out_shape, list)
    shapes = [jax.ShapeDtypeStruct(shape, jnp.bfloat16) for shape in (out_shape if several else [out_shape])]
    return pl.pallas_call(
        kernel,
        in_specs=[pl.BlockSpec(memory_space=pltpu.SMEM)] * len(scalars)
        + [near] * len(operands)
        + [pl.BlockSpec(memory_space=pltpu.HBM)] * len(far),
        out_specs=[near] * len(shapes) if several else near,
        out_shape=shapes if several else shapes[0],
        scratch_shapes=scratch,
        compiler_params=pltpu.CompilerParams(vmem_limit_bytes=20 * 2**20),
        cost_estimate=cost(flops, 2 * sum(operand.size for operand in (*operands, *far))),
        name=name,
    )(*scalars, *operands, *(pltpu.with_memory_space_constraint(each, pltpu.HBM) for each in far))


def buffer(*shape, dtype=jnp.bfloat16):
    return pltpu.VMEM(shape, dtype)


def first_gradients(heads, rates, keys, values, gate, up, down, depth):
    rows, width, units = keys.shape[0], *gate.shape[1:]
    held = [(rows, width), (rows, width), (width, units), (width, units), (units, width)]
    pieces = (depth, KINDS, width // depth, units)
    work = [buffer(rows, width)] + [buffer(rows, units)] * 3
    return in_vmem(
        first_head_kernel,
        "first_gradients",
        [pieces, *held],
        (heads,),
        (rates,),
        [buffer(*shape) for shape in held] + work + [pltpu.SemaphoreType.DMA((2, 5))],
        12 * rows * width * units,
        (keys, values, gate, up, down),
    )


def second_gradients(head, rates, lines, values, gate, up, down, depth):
    (rows, width), units = lines.shape, gate.shape[1]
    return in_vmem(
        second_head_kernel,
        "second_gradients",
        (depth, KINDS, width // depth, units),
        (head,),
        (rates, lines, values, gate, up, down),
        [buffer(rows, width)] + [buffer(rows, units)] * 3,
        12 * rows * width * units,
    )


def newton_schulz(blocks):
    count, rows, units = blocks.shape
    whole = buffer(rows, count * units)
    return in_vmem(
        newton_schulz_kernel,
        "newton_schulz",
        blocks.shape,
        (),
        (blocks,),
        [whole, whole, buffer(rows, rows), buffer(rows, rows, dtype=jnp.float32)],
        18 * rows * rows * count * units,
    )


def rescaled(head, head_rate, ortho, gate, up, down):
    width, units = gate.shape
    return in_vmem(
        rescale_kernel,
        "rescale",
        (KINDS, width, units),
        (head, head_rate),
        (ortho, gate, up, down),
        [],
        20 * KINDS * width * units,
    )


def query_terms(head, queries, weights, earlier=None):
    rows = queries.shape[0]
    _, width, units = weights.shape
    pieces = width // units
    return in_vmem(
        query_kernel,
        "query",
        (pieces if earlier is None else 2 * pieces, rows, units),
        (head,),
        (queries, weights) if earlier is None else (queries, weights, earlier),
        [],
        6 * rows * width * units,
    )


def local(queries, keys, values, token_rate, head_rate, w_gate, w_up, w_down):
    core = lax.axis_index("core").astype(jnp.int32)
    mine, theirs = core.reshape(1), (1 - core).reshape(1)
    swap = [(0, 1), (1, 0)]
    depth = lax.axis_size("z")
    rates = token_rate.T
    there, *held = first_gradients(
        jnp.stack((1 - core, core)), rates, keys, values, w_gate, w_up, w_down, depth
    )
    received = lax.ppermute(there, "core", swap)
    pieces = (
        second_gradients(mine, rates, *held, depth).astype(jnp.float32)
        + received.astype(jnp.float32)
    ).astype(jnp.bfloat16)
    owned = sum_of_copies(pieces, "z").astype(jnp.bfloat16)
    full = lax.all_gather(owned, "z", axis=1, tiled=True)
    blocks = lax.all_to_all(jnp.concatenate((full, full[:1]), axis=0), "hid", 0, 0, tiled=True)
    ortho = lax.all_to_all(newton_schulz(blocks), "hid", 0, 0, tiled=True)
    new = rescaled(mine, head_rate, ortho, *held[2:])
    new_there = lax.ppermute(new, "core", swap)
    terms = query_terms(theirs, queries, new_there, query_terms(mine, queries, new))
    return sum_of_copies(terms, "hid").astype(jnp.bfloat16)


def solution(mesh):
    finer = Mesh(
        mesh.devices.reshape(mesh.shape["head"], -1, 2, mesh.shape["hid"]),
        ("head", "z", "core", "hid"),
    )
    return jax.shard_map(
        local,
        mesh=finer,
        in_specs=(
            P(TOK, "head"),
            P(TOK, "head"),
            P(TOK, "head"),
            P(TOK, "head"),
            P("head"),
            P("head", None, "hid"),
            P("head", None, "hid"),
            P("head", "hid", None),
        ),
        out_specs=P(TOK, ("head", "hid")),
        check_vma=False,
    )
```

```python
import jax
import jax.numpy as jnp
from jax import lax
from jax.experimental import pallas as pl
from jax.experimental.pallas import tpu as pltpu
from jax.sharding import Mesh
from jax.sharding import PartitionSpec as P

NS_ITERS = 3
Z = ("far", "near")
TOK = (*Z, "core")
NEAR = 4
KINDS = 3
TILE = 128

poly_a = 3.4445
poly_b = -4.775
poly_c = 2.0315


def dot32(left, right, contract):
    return lax.dot_general(left, right, (contract, ((), ())), preferred_element_type=jnp.float32)


def sum_of_copies(pieces, axis):
    got = lax.all_to_all(pieces, axis, 0, 0, tiled=True)
    return jnp.sum(got.astype(jnp.float32), axis=0)


def sigmoid(value):
    return 1.0 / (1.0 + jnp.exp(-value))


def head_gradients(head, lines, values, rates, gate, up, down, out, target, d_gate, d_up, hidden):
    first = head == 0
    rows, width = lines.shape
    for start in range(0, rows, TILE):
        part = slice(start, start + TILE)
        rate = jnp.where(first, rates[0:1, part], rates[1:2, part])
        rate = jnp.broadcast_to(rate, (TILE, TILE)).T
        rate = jnp.concatenate([rate] * (width // TILE), axis=1)
        goal = (-(rate * values[part, :].astype(jnp.float32))).astype(jnp.bfloat16)
        target[part, :] = goal
        gate_pre = dot32(lines[part, :], gate[...], ((1,), (0,)))
        up_pre = dot32(lines[part, :], up[...], ((1,), (0,)))
        back = dot32(goal, down[...], ((1,), (1,)))
        gate_sig = sigmoid(gate_pre)
        active = gate_pre * gate_sig
        hidden[part, :] = (active * up_pre).astype(jnp.bfloat16)
        d_gate[part, :] = (back * up_pre * gate_sig * (1.0 + gate_pre * (1.0 - gate_sig))).astype(
            jnp.bfloat16
        )
        d_up[part, :] = (back * active).astype(jnp.bfloat16)
    depth, _, chunk, units = out.shape
    for kind, (left, right) in enumerate(((lines, d_gate), (lines, d_up), (target, hidden))):
        term = dot32(left[...], right[...], ((0,), (0,))).astype(jnp.bfloat16)
        out[:, kind] = term.reshape(depth, chunk, units)


def first_head_kernel(heads, keys, values, gate, up, down, all_rates, out, *rest):
    kept, rates, held, work, sems = rest[:5], rest[5], rest[6:11], rest[11:15], rest[15]
    width = held[0].shape[1]
    copies = [pltpu.make_async_copy(all_rates, rates, sems.at[2, 0])]
    copies[0].start()
    for turn, places in enumerate((held, kept)):
        head = heads[turn]
        columns = pl.ds(pl.multiple_of(head * width, width), width)
        sources = (keys.at[:, columns], values.at[:, columns], gate.at[head], up.at[head], down.at[head])
        for at, (source, place) in enumerate(zip(sources, places)):
            copy = pltpu.make_async_copy(source, place, sems.at[turn, at])
            copy.start()
            copies.append(copy)
    for copy in copies[:6]:
        copy.wait()
    lines, goals, own_gate, own_up, own_down = held
    head_gradients(heads[0], lines, goals, rates, own_gate, own_up, own_down, out, *work)
    for copy in copies[6:]:
        copy.wait()


def second_head_kernel(head_ref, rates, lines, values, gate, up, down, out, *work):
    head_gradients(head_ref[0], lines, values, rates, gate, up, down, out, *work)


def newton_schulz_kernel(blocks, out, iterate, gram, factor, raw):
    count, rows, units = blocks.shape
    columns = [slice(at * units, (at + 1) * units) for at in range(count)]
    halves = [slice(at, at + units) for at in range(0, rows, units)]
    for at in range(count):
        iterate[:, columns[at]] = blocks[at]
    scale = 1.0
    for iteration in range(NS_ITERS):
        if iteration == 0:
            trace = jnp.zeros((1, 1), jnp.float32)
            for half in halves:
                block = dot32(iterate[...], iterate[half, :], ((1,), (1,)))
                raw[:, half] = block
                square = block[half, :]
                line = lax.broadcasted_iota(jnp.int32, square.shape, 0)
                column = lax.broadcasted_iota(jnp.int32, square.shape, 1)
                trace = trace + jnp.sum(
                    jnp.where(line == column, square, 0.0), axis=(0, 1), keepdims=True
                )
            scale = 1.0 / (jnp.sqrt(trace) + 1e-07)
            for half in halves:
                gram[:, half] = (raw[:, half] * (scale * scale)).astype(jnp.bfloat16)
        else:
            for half in halves:
                gram[:, half] = dot32(iterate[...], iterate[half, :], ((1,), (1,))).astype(
                    jnp.bfloat16
                )
        for half in halves:
            square = dot32(gram[...], gram[:, half], ((1,), (0,)))
            factor[:, half] = (
                poly_b * gram[:, half].astype(jnp.float32) + poly_c * square
            ).astype(jnp.bfloat16)
        for at in range(count):
            current = iterate[:, columns[at]]
            block = poly_a * current.astype(jnp.float32) + dot32(
                factor[...], current, ((1,), (0,))
            )
            if iteration == 0:
                block = block * scale
            if iteration == NS_ITERS - 1:
                out[at] = block.astype(jnp.bfloat16)
            else:
                iterate[:, columns[at]] = block.astype(jnp.bfloat16)


def rescale_kernel(head_ref, head_rate, ortho, gate, up, down, out):
    step = head_rate[head_ref[0]]
    for kind in range(KINDS):
        if kind == 2:
            old = down[...].astype(jnp.float32).T
        else:
            old = (gate, up)[kind][...].astype(jnp.float32)
        fresh = old - step * ortho[kind].astype(jnp.float32)
        old_norm = jnp.sqrt(jnp.sum(old * old, axis=0, keepdims=True))
        new_norm = jnp.sqrt(jnp.sum(fresh * fresh, axis=0, keepdims=True) + 1e-06)
        out[kind] = (fresh * (old_norm / new_norm)).astype(jnp.bfloat16)


def query_kernel(head_ref, queries, weights, *rest):
    out = rest[-1]
    head = head_ref[0]
    _, width, units = weights.shape
    pieces = width // units
    rows = queries.shape[0]
    columns = pl.ds(pl.multiple_of(head * width, width), width)
    base = 0
    if len(rest) == 2:
        base = head * pieces
        out[pl.ds(pieces - base, pieces)] = rest[0][...]
    for start in range(0, rows, 2 * TILE):
        part = slice(start, start + 2 * TILE)
        lines = queries[part, columns]
        query_gate = dot32(lines, weights[0], ((1,), (0,)))
        query_up = dot32(lines, weights[1], ((1,), (0,)))
        query_hidden = (query_gate * sigmoid(query_gate) * query_up).astype(jnp.bfloat16)
        for at in range(pieces):
            features = weights[2, at * units : (at + 1) * units, :]
            out[base + at, part, :] = dot32(query_hidden, features, ((1,), (1,))).astype(
                jnp.bfloat16
            )


def cost(flops, operands):
    return pl.CostEstimate(flops=flops, transcendentals=0, bytes_accessed=operands)


def in_vmem(kernel, name, out_shape, scalars, operands, scratch, flops, far=()):
    near = pl.BlockSpec(memory_space=pltpu.VMEM)
    several = isinstance(out_shape, list)
    shapes = [
        jax.ShapeDtypeStruct(shape, jnp.float32 if len(shape) == 2 and shape[0] == 2 else jnp.bfloat16)
        for shape in (out_shape if several else [out_shape])
    ]
    return pl.pallas_call(
        kernel,
        in_specs=[pl.BlockSpec(memory_space=pltpu.SMEM)] * len(scalars)
        + [near] * len(operands)
        + [pl.BlockSpec(memory_space=pltpu.HBM)] * len(far),
        out_specs=[near] * len(shapes) if several else near,
        out_shape=shapes if several else shapes[0],
        scratch_shapes=scratch,
        compiler_params=pltpu.CompilerParams(vmem_limit_bytes=20 * 2**20),
        cost_estimate=cost(flops, 2 * sum(operand.size for operand in (*operands, *far))),
        name=name,
    )(*scalars, *operands, *(pltpu.with_memory_space_constraint(each, pltpu.HBM) for each in far))


def buffer(*shape, dtype=jnp.bfloat16):
    return pltpu.VMEM(shape, dtype)


def first_gradients(heads, rates, keys, values, gate, up, down, depth):
    rows, width, units = keys.shape[0], *gate.shape[1:]
    held = [(rows, width), (rows, width), (width, units), (width, units), (units, width)]
    pieces = (depth, KINDS, width // depth, units)
    work = [buffer(rows, width)] + [buffer(rows, units)] * 3
    return in_vmem(
        first_head_kernel,
        "first_gradients",
        [pieces, *held, rates.shape],
        (heads,),
        (),
        [buffer(*shape) for shape in held] + work + [pltpu.SemaphoreType.DMA((3, 5))],
        12 * rows * width * units,
        (keys, values, gate, up, down, rates),
    )


def second_gradients(head, rates, lines, values, gate, up, down, depth):
    (rows, width), units = lines.shape, gate.shape[1]
    return in_vmem(
        second_head_kernel,
        "second_gradients",
        (depth, KINDS, width // depth, units),
        (head,),
        (rates, lines, values, gate, up, down),
        [buffer(rows, width)] + [buffer(rows, units)] * 3,
        12 * rows * width * units,
    )


def newton_schulz(blocks):
    count, rows, units = blocks.shape
    return in_vmem(
        newton_schulz_kernel,
        "newton_schulz",
        blocks.shape,
        (),
        (blocks,),
        [
            buffer(rows, count * units),
            buffer(rows, rows),
            buffer(rows, rows),
            buffer(rows, rows, dtype=jnp.float32),
        ],
        12 * rows * rows * count * units + 6 * rows**3,
    )


def rescaled(head, head_rate, ortho, gate, up, down):
    width, units = gate.shape
    return in_vmem(
        rescale_kernel,
        "rescale",
        (KINDS, width, units),
        (head, head_rate),
        (ortho, gate, up, down),
        [],
        20 * KINDS * width * units,
    )


def query_terms(head, queries, weights, earlier=None):
    rows = queries.shape[0]
    _, width, units = weights.shape
    pieces = width // units
    return in_vmem(
        query_kernel,
        "query",
        (pieces if earlier is None else 2 * pieces, rows, units),
        (head,),
        (queries, weights) if earlier is None else (queries, weights, earlier),
        [],
        6 * rows * width * units,
    )


def local(queries, keys, values, token_rate, head_rate, w_gate, w_up, w_down):
    core = lax.axis_index("core").astype(jnp.int32)
    mine, theirs = core.reshape(1), (1 - core).reshape(1)
    swap = [(0, 1), (1, 0)]
    near, far, depth = lax.axis_size("near"), lax.axis_size("far"), lax.axis_size(Z)
    there, *held, rates = first_gradients(
        jnp.stack((1 - core, core)), token_rate.T, keys, values, w_gate, w_up, w_down, depth
    )
    received = lax.ppermute(there, "core", swap)
    pieces = (
        second_gradients(mine, rates, *held, depth).astype(jnp.float32)
        + received.astype(jnp.float32)
    ).astype(jnp.bfloat16)
    near_sum = sum_of_copies(pieces.reshape(near, far, *pieces.shape[1:]), "near")
    owned = sum_of_copies(near_sum.astype(jnp.bfloat16), "far").astype(jnp.bfloat16)
    full = lax.all_gather(owned, Z, axis=0).reshape(far, near, *owned.shape)
    full = full.transpose(2, 1, 0, 3, 4).reshape(KINDS, -1, owned.shape[-1])
    blocks = lax.all_to_all(jnp.concatenate((full, full[:1]), axis=0), "hid", 0, 0, tiled=True)
    ortho = lax.all_to_all(newton_schulz(blocks), "hid", 0, 0, tiled=True)
    new = rescaled(mine, head_rate, ortho, *held[2:])
    new_there = lax.ppermute(new, "core", swap)
    terms = query_terms(theirs, queries, new_there, query_terms(mine, queries, new))
    return sum_of_copies(terms, "hid").astype(jnp.bfloat16)


def solution(mesh):
    finer = Mesh(
        mesh.devices.reshape(mesh.shape["head"], -1, NEAR, 2, mesh.shape["hid"]),
        ("head", *TOK, "hid"),
    )
    return jax.shard_map(
        local,
        mesh=finer,
        in_specs=(
            P(TOK, "head"),
            P(TOK, "head"),
            P(TOK, "head"),
            P(TOK, "head"),
            P("head"),
            P("head", None, "hid"),
            P("head", None, "hid"),
            P("head", "hid", None),
        ),
        out_specs=P(TOK, ("head", "hid")),
        check_vma=False,
    )
```

```python
import jax
import jax.numpy as jnp
from jax import lax
from jax.experimental import pallas as pl
from jax.experimental.pallas import tpu as pltpu
from jax.sharding import Mesh
from jax.sharding import PartitionSpec as P

NS_ITERS = 3
TOK = ("far", "near", "core")
NEAR = 4
KINDS = 3
TILE = 128

poly_a = 3.4445
poly_b = -4.775
poly_c = 2.0315


def dot32(left, right, contract):
    return lax.dot_general(left, right, (contract, ((), ())), preferred_element_type=jnp.float32)


def sum_of_copies(pieces, axis):
    got = lax.all_to_all(pieces, axis, 0, 0, tiled=True)
    return jnp.sum(got.astype(jnp.float32), axis=0)


def sigmoid(value):
    return 1.0 / (1.0 + jnp.exp(-value))


def head_gradients(head, lines, values, rates, gate, up, down, out, target, d_gate, d_up, hidden):
    first = head == 0
    rows, width = lines.shape
    for start in range(0, rows, TILE):
        part = slice(start, start + TILE)
        rate = jnp.where(first, rates[0:1, part], rates[1:2, part])
        rate = jnp.broadcast_to(rate, (TILE, TILE)).T
        rate = jnp.concatenate([rate] * (width // TILE), axis=1)
        goal = (-(rate * values[part, :].astype(jnp.float32))).astype(jnp.bfloat16)
        target[part, :] = goal
        gate_pre = dot32(lines[part, :], gate[...], ((1,), (0,)))
        up_pre = dot32(lines[part, :], up[...], ((1,), (0,)))
        back = dot32(goal, down[...], ((1,), (1,)))
        gate_sig = sigmoid(gate_pre)
        active = gate_pre * gate_sig
        hidden[part, :] = (active * up_pre).astype(jnp.bfloat16)
        d_gate[part, :] = (back * up_pre * gate_sig * (1.0 + gate_pre * (1.0 - gate_sig))).astype(
            jnp.bfloat16
        )
        d_up[part, :] = (back * active).astype(jnp.bfloat16)
    depth, _, chunk, units = out.shape
    for kind, (left, right) in enumerate(((lines, d_gate), (lines, d_up), (target, hidden))):
        term = dot32(left[...], right[...], ((0,), (0,))).astype(jnp.bfloat16)
        out[:, kind] = term.reshape(depth, chunk, units)


def first_head_kernel(heads, keys, values, gate, up, down, all_rates, out, *rest):
    kept, rates, held, work, sems = rest[:5], rest[5], rest[6:11], rest[11:15], rest[15]
    width = held[0].shape[1]
    copies = [pltpu.make_async_copy(all_rates, rates, sems.at[2, 0])]
    copies[0].start()
    for turn, places in enumerate((held, kept)):
        head = heads[turn]
        columns = pl.ds(pl.multiple_of(head * width, width), width)
        sources = (keys.at[:, columns], values.at[:, columns], gate.at[head], up.at[head], down.at[head])
        for at, (source, place) in enumerate(zip(sources, places)):
            copy = pltpu.make_async_copy(source, place, sems.at[turn, at])
            copy.start()
            copies.append(copy)
    for copy in copies[:6]:
        copy.wait()
    lines, goals, own_gate, own_up, own_down = held
    head_gradients(heads[0], lines, goals, rates, own_gate, own_up, own_down, out, *work)
    for copy in copies[6:]:
        copy.wait()


def second_head_kernel(head_ref, rates, lines, values, gate, up, down, out, *work):
    head_gradients(head_ref[0], lines, values, rates, gate, up, down, out, *work)


def newton_schulz_kernel(blocks, out, iterate, gram, factor, raw):
    count, rows, units = blocks.shape
    columns = [slice(at * units, (at + 1) * units) for at in range(count)]
    halves = [slice(at, at + units) for at in range(0, rows, units)]
    for at in range(count):
        iterate[:, columns[at]] = blocks[at]
    scale = 1.0
    for iteration in range(NS_ITERS):
        if iteration == 0:
            trace = jnp.zeros((1, 1), jnp.float32)
            for half in halves:
                block = dot32(iterate[...], iterate[half, :], ((1,), (1,)))
                raw[:, half] = block
                square = block[half, :]
                line = lax.broadcasted_iota(jnp.int32, square.shape, 0)
                column = lax.broadcasted_iota(jnp.int32, square.shape, 1)
                trace = trace + jnp.sum(
                    jnp.where(line == column, square, 0.0), axis=(0, 1), keepdims=True
                )
            scale = 1.0 / (jnp.sqrt(trace) + 1e-07)
            for half in halves:
                gram[:, half] = (raw[:, half] * (scale * scale)).astype(jnp.bfloat16)
        else:
            for half in halves:
                gram[:, half] = dot32(iterate[...], iterate[half, :], ((1,), (1,))).astype(
                    jnp.bfloat16
                )
        for half in halves:
            square = dot32(gram[...], gram[:, half], ((1,), (0,)))
            factor[:, half] = (
                poly_b * gram[:, half].astype(jnp.float32) + poly_c * square
            ).astype(jnp.bfloat16)
        for at in range(count):
            current = iterate[:, columns[at]]
            block = poly_a * current.astype(jnp.float32) + dot32(
                factor[...], current, ((1,), (0,))
            )
            if iteration == 0:
                block = block * scale
            if iteration == NS_ITERS - 1:
                out[at] = block.astype(jnp.bfloat16)
            else:
                iterate[:, columns[at]] = block.astype(jnp.bfloat16)


def rescale_kernel(head_ref, head_rate, ortho, gate, up, down, out):
    step = head_rate[head_ref[0]]
    for kind in range(KINDS):
        if kind == 2:
            old = down[...].astype(jnp.float32).T
        else:
            old = (gate, up)[kind][...].astype(jnp.float32)
        fresh = old - step * ortho[kind].astype(jnp.float32)
        old_norm = jnp.sqrt(jnp.sum(old * old, axis=0, keepdims=True))
        new_norm = jnp.sqrt(jnp.sum(fresh * fresh, axis=0, keepdims=True) + 1e-06)
        out[kind] = (fresh * (old_norm / new_norm)).astype(jnp.bfloat16)


def query_kernel(head_ref, queries, weights, *rest):
    out = rest[-1]
    head = head_ref[0]
    _, width, units = weights.shape
    pieces = width // units
    rows = queries.shape[0]
    columns = pl.ds(pl.multiple_of(head * width, width), width)
    base = 0
    if len(rest) == 2:
        base = head * pieces
        out[pl.ds(pieces - base, pieces)] = rest[0][...]
    for start in range(0, rows, 2 * TILE):
        part = slice(start, start + 2 * TILE)
        lines = queries[part, columns]
        query_gate = dot32(lines, weights[0], ((1,), (0,)))
        query_up = dot32(lines, weights[1], ((1,), (0,)))
        query_hidden = (query_gate * sigmoid(query_gate) * query_up).astype(jnp.bfloat16)
        for at in range(pieces):
            features = weights[2, at * units : (at + 1) * units, :]
            out[base + at, part, :] = dot32(query_hidden, features, ((1,), (1,))).astype(
                jnp.bfloat16
            )


def cost(flops, operands):
    return pl.CostEstimate(flops=flops, transcendentals=0, bytes_accessed=operands)


def in_vmem(kernel, name, out_shape, scalars, operands, scratch, flops, far=()):
    near = pl.BlockSpec(memory_space=pltpu.VMEM)
    several = isinstance(out_shape, list)
    shapes = [
        jax.ShapeDtypeStruct(shape, jnp.float32 if len(shape) == 2 and shape[0] == 2 else jnp.bfloat16)
        for shape in (out_shape if several else [out_shape])
    ]
    return pl.pallas_call(
        kernel,
        in_specs=[pl.BlockSpec(memory_space=pltpu.SMEM)] * len(scalars)
        + [near] * len(operands)
        + [pl.BlockSpec(memory_space=pltpu.HBM)] * len(far),
        out_specs=[near] * len(shapes) if several else near,
        out_shape=shapes if several else shapes[0],
        scratch_shapes=scratch,
        compiler_params=pltpu.CompilerParams(vmem_limit_bytes=20 * 2**20),
        cost_estimate=cost(flops, 2 * sum(operand.size for operand in (*operands, *far))),
        name=name,
    )(*scalars, *operands, *(pltpu.with_memory_space_constraint(each, pltpu.HBM) for each in far))


def buffer(*shape, dtype=jnp.bfloat16):
    return pltpu.VMEM(shape, dtype)


def first_gradients(heads, rates, keys, values, gate, up, down, depth):
    rows, width, units = keys.shape[0], *gate.shape[1:]
    held = [(rows, width), (rows, width), (width, units), (width, units), (units, width)]
    pieces = (depth, KINDS, width // depth, units)
    work = [buffer(rows, width)] + [buffer(rows, units)] * 3
    return in_vmem(
        first_head_kernel,
        "first_gradients",
        [pieces, *held, rates.shape],
        (heads,),
        (),
        [buffer(*shape) for shape in held] + work + [pltpu.SemaphoreType.DMA((3, 5))],
        12 * rows * width * units,
        (keys, values, gate, up, down, rates),
    )


def second_gradients(head, rates, lines, values, gate, up, down, depth):
    (rows, width), units = lines.shape, gate.shape[1]
    return in_vmem(
        second_head_kernel,
        "second_gradients",
        (depth, KINDS, width // depth, units),
        (head,),
        (rates, lines, values, gate, up, down),
        [buffer(rows, width)] + [buffer(rows, units)] * 3,
        12 * rows * width * units,
    )


def newton_schulz(blocks):
    count, rows, units = blocks.shape
    return in_vmem(
        newton_schulz_kernel,
        "newton_schulz",
        blocks.shape,
        (),
        (blocks,),
        [
            buffer(rows, count * units),
            buffer(rows, rows),
            buffer(rows, rows),
            buffer(rows, rows, dtype=jnp.float32),
        ],
        12 * rows * rows * count * units + 6 * rows**3,
    )


def rescaled(head, head_rate, ortho, gate, up, down):
    width, units = gate.shape
    return in_vmem(
        rescale_kernel,
        "rescale",
        (KINDS, width, units),
        (head, head_rate),
        (ortho, gate, up, down),
        [],
        20 * KINDS * width * units,
    )


def query_terms(head, queries, weights, earlier=None):
    rows = queries.shape[0]
    _, width, units = weights.shape
    pieces = width // units
    return in_vmem(
        query_kernel,
        "query",
        (pieces if earlier is None else 2 * pieces, rows, units),
        (head,),
        (queries, weights) if earlier is None else (queries, weights, earlier),
        [],
        6 * rows * width * units,
    )


def local(queries, keys, values, token_rate, head_rate, w_gate, w_up, w_down):
    core = lax.axis_index("core").astype(jnp.int32)
    mine, theirs = core.reshape(1), (1 - core).reshape(1)
    swap = [(0, 1), (1, 0)]
    depth = lax.axis_size("near")
    there, *held, rates = first_gradients(
        jnp.stack((1 - core, core)), token_rate.T, keys, values, w_gate, w_up, w_down, depth
    )
    received = lax.ppermute(there, "core", swap)
    pieces = (
        second_gradients(mine, rates, *held, depth).astype(jnp.float32)
        + received.astype(jnp.float32)
    ).astype(jnp.bfloat16)
    near_sum = sum_of_copies(pieces, "near").astype(jnp.bfloat16)
    partials = lax.all_gather(near_sum, "far", axis=0)
    owned = jnp.sum(partials.astype(jnp.float32), axis=0).astype(jnp.bfloat16)
    full = lax.all_gather(owned, "near", axis=0)
    full = full.transpose(1, 0, 2, 3).reshape(KINDS, -1, owned.shape[-1])
    blocks = lax.all_to_all(jnp.concatenate((full, full[:1]), axis=0), "hid", 0, 0, tiled=True)
    ortho = lax.all_to_all(newton_schulz(blocks), "hid", 0, 0, tiled=True)
    new = rescaled(mine, head_rate, ortho, *held[2:])
    new_there = lax.ppermute(new, "core", swap)
    terms = query_terms(theirs, queries, new_there, query_terms(mine, queries, new))
    return sum_of_copies(terms, "hid").astype(jnp.bfloat16)


def solution(mesh):
    finer = Mesh(
        mesh.devices.reshape(mesh.shape["head"], -1, NEAR, 2, mesh.shape["hid"]),
        ("head", *TOK, "hid"),
    )
    return jax.shard_map(
        local,
        mesh=finer,
        in_specs=(
            P(TOK, "head"),
            P(TOK, "head"),
            P(TOK, "head"),
            P(TOK, "head"),
            P("head"),
            P("head", None, "hid"),
            P("head", None, "hid"),
            P("head", "hid", None),
        ),
        out_specs=P(TOK, ("head", "hid")),
        check_vma=False,
    )
```

```python
import jax
import jax.numpy as jnp
from jax import lax
from jax.experimental import pallas as pl
from jax.experimental.pallas import tpu as pltpu
from jax.sharding import Mesh
from jax.sharding import PartitionSpec as P

NS_ITERS = 3
TOK = ("far", "near", "core")
NEAR = 4
KINDS = 3
TILE = 128

poly_a = 3.4445
poly_b = -4.775
poly_c = 2.0315


def dot32(left, right, contract):
    return lax.dot_general(left, right, (contract, ((), ())), preferred_element_type=jnp.float32)


def sum_of_copies(pieces, axis):
    got = lax.all_to_all(pieces, axis, 0, 0, tiled=True)
    return jnp.sum(got.astype(jnp.float32), axis=0)


def sigmoid(value):
    return 1.0 / (1.0 + jnp.exp(-value))


def head_gradients(
    head, lines, values, rates, gate, up, down, out, target, d_gate, d_up, hidden, before=None
):
    first = head == 0
    rows, width = lines.shape
    for start in range(0, rows, TILE):
        part = slice(start, start + TILE)
        if before is not None:
            before(start // TILE)
        rate = jnp.where(first, rates[0:1, part], rates[1:2, part])
        rate = jnp.broadcast_to(rate, (TILE, TILE)).T
        rate = jnp.concatenate([rate] * (width // TILE), axis=1)
        goal = (-(rate * values[part, :].astype(jnp.float32))).astype(jnp.bfloat16)
        target[part, :] = goal
        gate_pre = dot32(lines[part, :], gate[...], ((1,), (0,)))
        up_pre = dot32(lines[part, :], up[...], ((1,), (0,)))
        back = dot32(goal, down[...], ((1,), (1,)))
        gate_sig = sigmoid(gate_pre)
        active = gate_pre * gate_sig
        hidden[part, :] = (active * up_pre).astype(jnp.bfloat16)
        d_gate[part, :] = (back * up_pre * gate_sig * (1.0 + gate_pre * (1.0 - gate_sig))).astype(
            jnp.bfloat16
        )
        d_up[part, :] = (back * active).astype(jnp.bfloat16)
    depth, _, chunk, units = out.shape
    for kind, (left, right) in enumerate(((lines, d_gate), (lines, d_up), (target, hidden))):
        term = dot32(left[...], right[...], ((0,), (0,))).astype(jnp.bfloat16)
        out[:, kind] = term.reshape(depth, chunk, units)


def first_head_kernel(heads, keys, values, gate, up, down, all_rates, out, *rest):
    kept, rates, held, work, sems = rest[:5], rest[5], rest[6:11], rest[11:15], rest[15]
    rows, width = held[0].shape
    parts = [pl.ds(start, min(TILE, rows)) for start in range(0, rows, TILE)]

    def sources(turn):
        columns = pl.ds(pl.multiple_of(heads[turn] * width, width), width)
        return columns, [each.at[heads[turn]] for each in (gate, up, down)]

    columns, weights = sources(0)
    loads = list(zip((all_rates, *weights), (rates, *held[2:])))
    for part in parts:
        for whole, place in zip((keys, values), held):
            loads.append((whole.at[part, columns], place.at[part, :]))
    loads = [
        pltpu.make_async_copy(source, place, sems.at[0, at])
        for at, (source, place) in enumerate(loads)
    ]
    columns, weights = sources(1)
    later = [
        pltpu.make_async_copy(source, place, sems.at[1, at])
        for at, (source, place) in enumerate(
            zip((keys.at[:, columns], values.at[:, columns], *weights), kept)
        )
    ]
    for load in loads:
        load.start()

    def before(step):
        for load in loads[:6] if step == 0 else loads[4 + 2 * step : 6 + 2 * step]:
            load.wait()
        if step == 0:
            for load in later:
                load.start()

    lines, goals, own_gate, own_up, own_down = held
    head_gradients(
        heads[0], lines, goals, rates, own_gate, own_up, own_down, out, *work, before=before
    )
    for load in later:
        load.wait()


def second_head_kernel(head_ref, rates, lines, values, gate, up, down, out, *work):
    head_gradients(head_ref[0], lines, values, rates, gate, up, down, out, *work)


def newton_schulz_kernel(blocks, out, iterate, gram, factor, raw):
    count, rows, units = blocks.shape
    columns = [slice(at * units, (at + 1) * units) for at in range(count)]
    halves = [slice(at, at + units) for at in range(0, rows, units)]
    for at in range(count):
        iterate[:, columns[at]] = blocks[at]
    scale = 1.0
    for iteration in range(NS_ITERS):
        if iteration == 0:
            trace = jnp.zeros((1, 1), jnp.float32)
            for half in halves:
                block = dot32(iterate[...], iterate[half, :], ((1,), (1,)))
                raw[:, half] = block
                square = block[half, :]
                line = lax.broadcasted_iota(jnp.int32, square.shape, 0)
                column = lax.broadcasted_iota(jnp.int32, square.shape, 1)
                trace = trace + jnp.sum(
                    jnp.where(line == column, square, 0.0), axis=(0, 1), keepdims=True
                )
            scale = 1.0 / (jnp.sqrt(trace) + 1e-07)
            for half in halves:
                gram[:, half] = (raw[:, half] * (scale * scale)).astype(jnp.bfloat16)
        else:
            for half in halves:
                gram[:, half] = dot32(iterate[...], iterate[half, :], ((1,), (1,))).astype(
                    jnp.bfloat16
                )
        for half in halves:
            square = dot32(gram[...], gram[:, half], ((1,), (0,)))
            factor[:, half] = (
                poly_b * gram[:, half].astype(jnp.float32) + poly_c * square
            ).astype(jnp.bfloat16)
        for at in range(count):
            current = iterate[:, columns[at]]
            block = poly_a * current.astype(jnp.float32) + dot32(
                factor[...], current, ((1,), (0,))
            )
            if iteration == 0:
                block = block * scale
            if iteration == NS_ITERS - 1:
                out[at] = block.astype(jnp.bfloat16)
            else:
                iterate[:, columns[at]] = block.astype(jnp.bfloat16)


def rescale_kernel(head_ref, head_rate, ortho, gate, up, down, out):
    step = head_rate[head_ref[0]]
    for kind in range(KINDS):
        if kind == 2:
            old = down[...].astype(jnp.float32).T
        else:
            old = (gate, up)[kind][...].astype(jnp.float32)
        fresh = old - step * ortho[kind].astype(jnp.float32)
        old_norm = jnp.sqrt(jnp.sum(old * old, axis=0, keepdims=True))
        new_norm = jnp.sqrt(jnp.sum(fresh * fresh, axis=0, keepdims=True) + 1e-06)
        out[kind] = (fresh * (old_norm / new_norm)).astype(jnp.bfloat16)


def query_kernel(head_ref, queries, weights, *rest):
    out = rest[-1]
    head = head_ref[0]
    _, width, units = weights.shape
    pieces = width // units
    rows = queries.shape[0]
    columns = pl.ds(pl.multiple_of(head * width, width), width)
    base = 0
    if len(rest) == 2:
        base = head * pieces
        out[pl.ds(pieces - base, pieces)] = rest[0][...]
    for start in range(0, rows, 2 * TILE):
        part = slice(start, start + 2 * TILE)
        lines = queries[part, columns]
        query_gate = dot32(lines, weights[0], ((1,), (0,)))
        query_up = dot32(lines, weights[1], ((1,), (0,)))
        query_hidden = (query_gate * sigmoid(query_gate) * query_up).astype(jnp.bfloat16)
        for at in range(pieces):
            features = weights[2, at * units : (at + 1) * units, :]
            out[base + at, part, :] = dot32(query_hidden, features, ((1,), (1,))).astype(
                jnp.bfloat16
            )


def cost(flops, operands):
    return pl.CostEstimate(flops=flops, transcendentals=0, bytes_accessed=operands)


def in_vmem(kernel, name, out_shape, scalars, operands, scratch, flops, far=()):
    near = pl.BlockSpec(memory_space=pltpu.VMEM)
    several = isinstance(out_shape, list)
    shapes = [
        jax.ShapeDtypeStruct(shape, jnp.float32 if len(shape) == 2 and shape[0] == 2 else jnp.bfloat16)
        for shape in (out_shape if several else [out_shape])
    ]
    return pl.pallas_call(
        kernel,
        in_specs=[pl.BlockSpec(memory_space=pltpu.SMEM)] * len(scalars)
        + [near] * len(operands)
        + [pl.BlockSpec(memory_space=pltpu.HBM)] * len(far),
        out_specs=[near] * len(shapes) if several else near,
        out_shape=shapes if several else shapes[0],
        scratch_shapes=scratch,
        compiler_params=pltpu.CompilerParams(vmem_limit_bytes=20 * 2**20),
        cost_estimate=cost(flops, 2 * sum(operand.size for operand in (*operands, *far))),
        name=name,
    )(*scalars, *operands, *(pltpu.with_memory_space_constraint(each, pltpu.HBM) for each in far))


def buffer(*shape, dtype=jnp.bfloat16):
    return pltpu.VMEM(shape, dtype)


def first_gradients(heads, rates, keys, values, gate, up, down, depth):
    rows, width, units = keys.shape[0], *gate.shape[1:]
    held = [(rows, width), (rows, width), (width, units), (width, units), (units, width)]
    pieces = (depth, KINDS, width // depth, units)
    work = [buffer(rows, width)] + [buffer(rows, units)] * 3
    return in_vmem(
        first_head_kernel,
        "first_gradients",
        [pieces, *held, rates.shape],
        (heads,),
        (),
        [buffer(*shape) for shape in held] + work + [pltpu.SemaphoreType.DMA((2, 4 + 2 * pl.cdiv(rows, TILE)))],
        12 * rows * width * units,
        (keys, values, gate, up, down, rates),
    )


def second_gradients(head, rates, lines, values, gate, up, down, depth):
    (rows, width), units = lines.shape, gate.shape[1]
    return in_vmem(
        second_head_kernel,
        "second_gradients",
        (depth, KINDS, width // depth, units),
        (head,),
        (rates, lines, values, gate, up, down),
        [buffer(rows, width)] + [buffer(rows, units)] * 3,
        12 * rows * width * units,
    )


def newton_schulz(blocks):
    count, rows, units = blocks.shape
    return in_vmem(
        newton_schulz_kernel,
        "newton_schulz",
        blocks.shape,
        (),
        (blocks,),
        [
            buffer(rows, count * units),
            buffer(rows, rows),
            buffer(rows, rows),
            buffer(rows, rows, dtype=jnp.float32),
        ],
        12 * rows * rows * count * units + 6 * rows**3,
    )


def rescaled(head, head_rate, ortho, gate, up, down):
    width, units = gate.shape
    return in_vmem(
        rescale_kernel,
        "rescale",
        (KINDS, width, units),
        (head, head_rate),
        (ortho, gate, up, down),
        [],
        20 * KINDS * width * units,
    )


def query_terms(head, queries, weights, earlier=None):
    rows = queries.shape[0]
    _, width, units = weights.shape
    pieces = width // units
    return in_vmem(
        query_kernel,
        "query",
        (pieces if earlier is None else 2 * pieces, rows, units),
        (head,),
        (queries, weights) if earlier is None else (queries, weights, earlier),
        [],
        6 * rows * width * units,
    )


def local(queries, keys, values, token_rate, head_rate, w_gate, w_up, w_down):
    core = lax.axis_index("core").astype(jnp.int32)
    mine, theirs = core.reshape(1), (1 - core).reshape(1)
    swap = [(0, 1), (1, 0)]
    depth = lax.axis_size("near")
    there, *held, rates = first_gradients(
        jnp.stack((1 - core, core)), token_rate.T, keys, values, w_gate, w_up, w_down, depth
    )
    received = lax.ppermute(there, "core", swap)
    pieces = (
        second_gradients(mine, rates, *held, depth).astype(jnp.float32)
        + received.astype(jnp.float32)
    ).astype(jnp.bfloat16)
    near_sum = sum_of_copies(pieces, "near").astype(jnp.bfloat16)
    partials = lax.all_gather(near_sum, "far", axis=0)
    owned = jnp.sum(partials.astype(jnp.float32), axis=0).astype(jnp.bfloat16)
    full = lax.all_gather(owned, "near", axis=1, tiled=True)
    blocks = lax.all_to_all(jnp.concatenate((full, full[:1]), axis=0), "hid", 0, 0, tiled=True)
    ortho = lax.all_to_all(newton_schulz(blocks), "hid", 0, 0, tiled=True)
    new = rescaled(mine, head_rate, ortho, *held[2:])
    new_there = lax.ppermute(new, "core", swap)
    terms = query_terms(theirs, queries, new_there, query_terms(mine, queries, new))
    return sum_of_copies(terms, "hid").astype(jnp.bfloat16)


def solution(mesh):
    finer = Mesh(
        mesh.devices.reshape(mesh.shape["head"], -1, NEAR, 2, mesh.shape["hid"]),
        ("head", *TOK, "hid"),
    )
    return jax.shard_map(
        local,
        mesh=finer,
        in_specs=(
            P(TOK, "head"),
            P(TOK, "head"),
            P(TOK, "head"),
            P(TOK, "head"),
            P("head"),
            P("head", None, "hid"),
            P("head", None, "hid"),
            P("head", "hid", None),
        ),
        out_specs=P(TOK, ("head", "hid")),
        check_vma=False,
    )
```

```python
import jax
import jax.numpy as jnp
from jax import lax
from jax.experimental import pallas as pl
from jax.experimental.pallas import tpu as pltpu
from jax.sharding import Mesh
from jax.sharding import PartitionSpec as P

NS_ITERS = 3
TOK = ("far", "near", "core")
NEAR = 4
KINDS = 3
TILE = 128

poly_a = 3.4445
poly_b = -4.775
poly_c = 2.0315


def dot32(left, right, contract):
    return lax.dot_general(left, right, (contract, ((), ())), preferred_element_type=jnp.float32)


def sum_of_copies(pieces, axis):
    got = lax.all_to_all(pieces, axis, 0, 0, tiled=True)
    return jnp.sum(got.astype(jnp.float32), axis=0)


def sigmoid(value):
    return 1.0 / (1.0 + jnp.exp(-value))


def head_gradients(head, lines, values, rates, gate, up, down, out, target, d_gate, d_up, hidden):
    first = head == 0
    rows, width = lines.shape
    for start in range(0, rows, TILE):
        part = slice(start, start + TILE)
        rate = jnp.where(first, rates[0:1, part], rates[1:2, part])
        rate = jnp.broadcast_to(rate, (TILE, TILE)).T
        rate = jnp.concatenate([rate] * (width // TILE), axis=1)
        goal = (-(rate * values[part, :].astype(jnp.float32))).astype(jnp.bfloat16)
        target[part, :] = goal
        gate_pre = dot32(lines[part, :], gate[...], ((1,), (0,)))
        up_pre = dot32(lines[part, :], up[...], ((1,), (0,)))
        back = dot32(goal, down[...], ((1,), (1,)))
        gate_sig = sigmoid(gate_pre)
        active = gate_pre * gate_sig
        hidden[part, :] = (active * up_pre).astype(jnp.bfloat16)
        d_gate[part, :] = (back * up_pre * gate_sig * (1.0 + gate_pre * (1.0 - gate_sig))).astype(
            jnp.bfloat16
        )
        d_up[part, :] = (back * active).astype(jnp.bfloat16)
    depth, _, chunk, units = out.shape
    for kind, (left, right) in enumerate(((lines, d_gate), (lines, d_up), (target, hidden))):
        term = dot32(left[...], right[...], ((0,), (0,))).astype(jnp.bfloat16)
        out[:, kind] = term.reshape(depth, chunk, units)


def first_head_kernel(heads, keys, values, gate, up, down, all_rates, out, *rest):
    kept, rates, held, work, sems = rest[:5], rest[5], rest[6:11], rest[11:15], rest[15]
    width = held[0].shape[1]
    copies = [pltpu.make_async_copy(all_rates, rates, sems.at[2, 0])]
    copies[0].start()
    for turn, places in enumerate((held, kept)):
        head = heads[turn]
        columns = pl.ds(pl.multiple_of(head * width, width), width)
        sources = (keys.at[:, columns], values.at[:, columns], gate.at[head], up.at[head], down.at[head])
        for at, (source, place) in enumerate(zip(sources, places)):
            copy = pltpu.make_async_copy(source, place, sems.at[turn, at])
            if turn == 0:
                copy.start()
            copies.append(copy)
    for copy in copies[:6]:
        copy.wait()
    for copy in copies[6:]:
        copy.start()
    lines, goals, own_gate, own_up, own_down = held
    head_gradients(heads[0], lines, goals, rates, own_gate, own_up, own_down, out, *work)
    for copy in copies[6:]:
        copy.wait()


def second_head_kernel(head_ref, rates, lines, values, gate, up, down, out, *work):
    head_gradients(head_ref[0], lines, values, rates, gate, up, down, out, *work)


def newton_schulz_kernel(blocks, out, iterate, gram, factor, raw):
    count, rows, units = blocks.shape
    columns = [slice(at * units, (at + 1) * units) for at in range(count)]
    halves = [slice(at, at + units) for at in range(0, rows, units)]
    for at in range(count):
        iterate[:, columns[at]] = blocks[at]
    scale = 1.0
    for iteration in range(NS_ITERS):
        if iteration == 0:
            trace = jnp.zeros((1, 1), jnp.float32)
            for half in halves:
                block = dot32(iterate[...], iterate[half, :], ((1,), (1,)))
                raw[:, half] = block
                square = block[half, :]
                line = lax.broadcasted_iota(jnp.int32, square.shape, 0)
                column = lax.broadcasted_iota(jnp.int32, square.shape, 1)
                trace = trace + jnp.sum(
                    jnp.where(line == column, square, 0.0), axis=(0, 1), keepdims=True
                )
            scale = 1.0 / (jnp.sqrt(trace) + 1e-07)
            for half in halves:
                gram[:, half] = (raw[:, half] * (scale * scale)).astype(jnp.bfloat16)
        else:
            for half in halves:
                gram[:, half] = dot32(iterate[...], iterate[half, :], ((1,), (1,))).astype(
                    jnp.bfloat16
                )
        for half in halves:
            square = dot32(gram[...], gram[:, half], ((1,), (0,)))
            factor[:, half] = (
                poly_b * gram[:, half].astype(jnp.float32) + poly_c * square
            ).astype(jnp.bfloat16)
        for at in range(count):
            current = iterate[:, columns[at]]
            block = poly_a * current.astype(jnp.float32) + dot32(
                factor[...], current, ((1,), (0,))
            )
            if iteration == 0:
                block = block * scale
            if iteration == NS_ITERS - 1:
                out[at] = block.astype(jnp.bfloat16)
            else:
                iterate[:, columns[at]] = block.astype(jnp.bfloat16)


def rescale_kernel(head_ref, head_rate, ortho, gate, up, down, out):
    step = head_rate[head_ref[0]]
    for kind in range(KINDS):
        if kind == 2:
            old = down[...].astype(jnp.float32).T
        else:
            old = (gate, up)[kind][...].astype(jnp.float32)
        fresh = old - step * ortho[kind].astype(jnp.float32)
        old_norm = jnp.sqrt(jnp.sum(old * old, axis=0, keepdims=True))
        new_norm = jnp.sqrt(jnp.sum(fresh * fresh, axis=0, keepdims=True) + 1e-06)
        out[kind] = (fresh * (old_norm / new_norm)).astype(jnp.bfloat16)


def query_kernel(head_ref, queries, weights, *rest):
    out = rest[-1]
    head = head_ref[0]
    _, width, units = weights.shape
    pieces = width // units
    rows = queries.shape[0]
    columns = pl.ds(pl.multiple_of(head * width, width), width)
    base = 0
    if len(rest) == 2:
        base = head * pieces
        out[pl.ds(pieces - base, pieces)] = rest[0][...]
    for start in range(0, rows, 2 * TILE):
        part = slice(start, start + 2 * TILE)
        lines = queries[part, columns]
        query_gate = dot32(lines, weights[0], ((1,), (0,)))
        query_up = dot32(lines, weights[1], ((1,), (0,)))
        query_hidden = (query_gate * sigmoid(query_gate) * query_up).astype(jnp.bfloat16)
        for at in range(pieces):
            features = weights[2, at * units : (at + 1) * units, :]
            out[base + at, part, :] = dot32(query_hidden, features, ((1,), (1,))).astype(
                jnp.bfloat16
            )


def cost(flops, operands):
    return pl.CostEstimate(flops=flops, transcendentals=0, bytes_accessed=operands)


def in_vmem(kernel, name, out_shape, scalars, operands, scratch, flops, far=()):
    near = pl.BlockSpec(memory_space=pltpu.VMEM)
    several = isinstance(out_shape, list)
    shapes = [
        jax.ShapeDtypeStruct(shape, jnp.float32 if len(shape) == 2 and shape[0] == 2 else jnp.bfloat16)
        for shape in (out_shape if several else [out_shape])
    ]
    return pl.pallas_call(
        kernel,
        in_specs=[pl.BlockSpec(memory_space=pltpu.SMEM)] * len(scalars)
        + [near] * len(operands)
        + [pl.BlockSpec(memory_space=pltpu.HBM)] * len(far),
        out_specs=[near] * len(shapes) if several else near,
        out_shape=shapes if several else shapes[0],
        scratch_shapes=scratch,
        compiler_params=pltpu.CompilerParams(vmem_limit_bytes=20 * 2**20),
        cost_estimate=cost(flops, 2 * sum(operand.size for operand in (*operands, *far))),
        name=name,
    )(*scalars, *operands, *(pltpu.with_memory_space_constraint(each, pltpu.HBM) for each in far))


def buffer(*shape, dtype=jnp.bfloat16):
    return pltpu.VMEM(shape, dtype)


def first_gradients(heads, rates, keys, values, gate, up, down, depth):
    rows, width, units = keys.shape[0], *gate.shape[1:]
    held = [(rows, width), (rows, width), (width, units), (width, units), (units, width)]
    pieces = (depth, KINDS, width // depth, units)
    work = [buffer(rows, width)] + [buffer(rows, units)] * 3
    return in_vmem(
        first_head_kernel,
        "first_gradients",
        [pieces, *held, rates.shape],
        (heads,),
        (),
        [buffer(*shape) for shape in held] + work + [pltpu.SemaphoreType.DMA((3, 5))],
        12 * rows * width * units,
        (keys, values, gate, up, down, rates),
    )


def second_gradients(head, rates, lines, values, gate, up, down, depth):
    (rows, width), units = lines.shape, gate.shape[1]
    return in_vmem(
        second_head_kernel,
        "second_gradients",
        (depth, KINDS, width // depth, units),
        (head,),
        (rates, lines, values, gate, up, down),
        [buffer(rows, width)] + [buffer(rows, units)] * 3,
        12 * rows * width * units,
    )


def newton_schulz(blocks):
    count, rows, units = blocks.shape
    return in_vmem(
        newton_schulz_kernel,
        "newton_schulz",
        blocks.shape,
        (),
        (blocks,),
        [
            buffer(rows, count * units),
            buffer(rows, rows),
            buffer(rows, rows),
            buffer(rows, rows, dtype=jnp.float32),
        ],
        12 * rows * rows * count * units + 6 * rows**3,
    )


def rescaled(head, head_rate, ortho, gate, up, down):
    width, units = gate.shape
    return in_vmem(
        rescale_kernel,
        "rescale",
        (KINDS, width, units),
        (head, head_rate),
        (ortho, gate, up, down),
        [],
        20 * KINDS * width * units,
    )


def query_terms(head, queries, weights, earlier=None):
    rows = queries.shape[0]
    _, width, units = weights.shape
    pieces = width // units
    return in_vmem(
        query_kernel,
        "query",
        (pieces if earlier is None else 2 * pieces, rows, units),
        (head,),
        (queries, weights) if earlier is None else (queries, weights, earlier),
        [],
        6 * rows * width * units,
    )


def local(queries, keys, values, token_rate, head_rate, w_gate, w_up, w_down):
    core = lax.axis_index("core").astype(jnp.int32)
    mine, theirs = core.reshape(1), (1 - core).reshape(1)
    swap = [(0, 1), (1, 0)]
    depth = lax.axis_size("near")
    there, *held, rates = first_gradients(
        jnp.stack((1 - core, core)), token_rate.T, keys, values, w_gate, w_up, w_down, depth
    )
    received = lax.ppermute(there, "core", swap)
    pieces = (
        second_gradients(mine, rates, *held, depth).astype(jnp.float32)
        + received.astype(jnp.float32)
    ).astype(jnp.bfloat16)
    near_sum = sum_of_copies(pieces, "near").astype(jnp.bfloat16)
    partials = lax.all_gather(near_sum, "far", axis=0)
    owned = jnp.sum(partials.astype(jnp.float32), axis=0).astype(jnp.bfloat16)
    full = lax.all_gather(owned, "near", axis=1, tiled=True)
    blocks = lax.all_to_all(jnp.concatenate((full, full[:1]), axis=0), "hid", 0, 0, tiled=True)
    ortho = lax.all_to_all(newton_schulz(blocks), "hid", 0, 0, tiled=True)
    new = rescaled(mine, head_rate, ortho, *held[2:])
    new_there = lax.ppermute(new, "core", swap)
    terms = query_terms(theirs, queries, new_there, query_terms(mine, queries, new))
    return sum_of_copies(terms, "hid").astype(jnp.bfloat16)


def solution(mesh):
    finer = Mesh(
        mesh.devices.reshape(mesh.shape["head"], -1, NEAR, 2, mesh.shape["hid"]),
        ("head", *TOK, "hid"),
    )
    return jax.shard_map(
        local,
        mesh=finer,
        in_specs=(
            P(TOK, "head"),
            P(TOK, "head"),
            P(TOK, "head"),
            P(TOK, "head"),
            P("head"),
            P("head", None, "hid"),
            P("head", None, "hid"),
            P("head", "hid", None),
        ),
        out_specs=P(TOK, ("head", "hid")),
        check_vma=False,
    )
```
